128 devices in a mesh: child: 2 (over core), rows: 64 (over z, y, x).
Axes of the slice: x: 4, y: 4, z: 4, core: 2. Of those that a mesh axis runs over, the one named last changes fastest.
Arguments:
- front_update: bfloat16 [2, 12288, 61440], P('child', 'rows'), may hold values from -0.0234375 to 0.0234375
- child_omega: bfloat16 [2, 61440, 256], P('child', 'rows'), may hold values from -6 to 6
- parent_block: bfloat16 [49152, 128], P(('child', 'rows')), may hold values from -0.5 to 0.5
- parent_omega: bfloat16 [49152, 256], P(('child', 'rows')), may hold values from -6 to 6
- child_map: int32 [2, 12288], replicated, may hold values from 0 to 49151, as said below
- leaf_order: int32 [49152], replicated, may hold values from 0 to 49151, as said below
Outputs:
- parent_samples: float32 [49152, 256], P(('child', 'rows'))
The draws below stay inside these ranges and needn't reach their ends.
Inputs may be any that keep to these rules, and one draw needn't show every extreme that they name: `child_map`: within one child the entries are distinct. Of each aligned block of 192 rows of one child, at most 3 entries fall in any one aligned block of 384 parent rows, and some block of parent rows gets exactly 3 from every such block. `leaf_order`: A permutation. Each aligned block of 384 leaf positions holds exactly 3 rows of every aligned block of 384 natural rows.
All inputs are finite; a program needn't handle non-finite values.
Results may differ from the reference program's by a relative error of at most 0.0003.
Values may be sent and summed in bfloat16 or wider, within the bound.
A program may use at most 192 MiB of HBM per device.

```python
import jax
import jax.numpy as jnp
from jax import lax

ORDER = 61440
SAMPLES = 256
BLOCK = 128
ROWS_DEV = 192
OWNERS = 128
PARENT_DEV = 384
CHILD_ROWS = 12288
PARENT_ROWS = 49152
CAP = 3
LEAF_CAP = 3
N_CHILD = 2
N_ROWS = 64


def draw_child_map(key, part):
    base = jax.random.fold_in(key, 11)
    key_weight, key_forced, key_score, key_shuffle, key_local = jax.random.split(base, 5)
    slot_total = OWNERS * CAP
    slot_owner = jnp.arange(slot_total, dtype=jnp.int32) // CAP
    weights = jax.random.randint(key_weight, (OWNERS,), 1, 5)
    forced = jax.random.randint(key_forced, (), 0, OWNERS)
    raw_scores = jax.random.randint(key_score, (OWNERS, slot_total), 0, 262144)
    scores = raw_scores // weights[slot_owner][None, :]
    scores = jnp.where(slot_owner[None, :] == forced, -1, scores)
    scores = scores * slot_total + jnp.arange(slot_total, dtype=jnp.int32)[None, :]
    chosen = jnp.argsort(scores, axis=1, stable=True)[:, :ROWS_DEV]
    shuffle_keys = jax.random.randint(key_shuffle, (OWNERS, ROWS_DEV), 0, 65536) * ROWS_DEV + jnp.arange(ROWS_DEV, dtype=jnp.int32)[None, :]
    shuffle = jnp.argsort(shuffle_keys, axis=1, stable=True)
    chosen = jnp.take_along_axis(chosen, shuffle, axis=1)
    target_owner = (chosen // CAP).astype(jnp.int32).reshape(N_CHILD, N_ROWS * ROWS_DEV)
    one_hot = (target_owner[:, :, None] == jnp.arange(OWNERS, dtype=jnp.int32)[None, None, :]).astype(jnp.int32)
    arrival_rank = jnp.sum(one_hot * jnp.cumsum(one_hot, axis=1), axis=2) - 1
    local_keys = jax.random.randint(key_local, (N_CHILD, OWNERS, PARENT_DEV), 0, 65536) * PARENT_DEV + jnp.arange(PARENT_DEV, dtype=jnp.int32)[None, None, :]
    local_perm = jnp.argsort(local_keys, axis=2, stable=True).astype(jnp.int32)
    flat_index = (jnp.arange(N_CHILD, dtype=jnp.int32)[:, None] * OWNERS + target_owner) * PARENT_DEV + arrival_rank
    local_row = local_perm.reshape(-1)[flat_index]
    return (target_owner * PARENT_DEV + local_row).astype(jnp.int32)


def draw_leaf_order(key, part):
    base = jax.random.fold_in(key, 23)
    key_spread, key_place = jax.random.split(base, 2)
    counter = jnp.arange(PARENT_DEV, dtype=jnp.int32)[None, :]
    spread_keys = jax.random.randint(key_spread, (OWNERS, PARENT_DEV), 0, 65536) * PARENT_DEV + counter
    spread = jnp.argsort(spread_keys, axis=1, stable=True).astype(jnp.int32)
    place_keys = jax.random.randint(key_place, (OWNERS, PARENT_DEV), 0, 65536) * PARENT_DEV + counter
    place = jnp.argsort(place_keys, axis=1, stable=True).astype(jnp.int32)
    natural_owner = jnp.arange(OWNERS, dtype=jnp.int32)[:, None]
    leaf_owner = (natural_owner + spread % OWNERS) % OWNERS
    copy_index = spread // OWNERS
    leaf_local = place.reshape(-1)[leaf_owner * PARENT_DEV + LEAF_CAP * natural_owner + copy_index]
    leaf_position = leaf_owner * PARENT_DEV + leaf_local
    natural_row = natural_owner * PARENT_DEV + counter
    return jnp.zeros((PARENT_ROWS,), jnp.int32).at[leaf_position.reshape(-1)].set(natural_row.reshape(-1))


def steps_of(own_key, dims, pieces, low, largest):
    def one(position, shards_of):
        draws = jax.random.uniform(jax.random.fold_in(jax.random.fold_in(own_key, 6), position), (shards_of,), jnp.float32, low / len(pieces), largest / len(pieces))
        return jnp.repeat(jnp.exp(draws), dims[position] // shards_of).reshape((-1,) + (1,) * (len(dims) - position - 1))

    level = one(*pieces[0])
    for cut in pieces[1:]:
        level = level * one(*cut)
    return level


def centred(stream_key, shape, scale, bound, cuts=(), kind=jnp.bfloat16):
    result = jax.random.normal(stream_key, shape, jnp.float32) * scale
    if len(cuts) > 0:
        result = steps_of(stream_key, shape, cuts, -0.22, 0.18) * result
    return jnp.clip(result, min=-bound, max=bound).astype(kind)


def setup_inputs(seed: int = 0) -> dict:
    keys = jax.random.split(jax.random.key(seed), 7)
    return {
        "front_update": centred(keys[0], (N_CHILD, CHILD_ROWS, ORDER), ORDER ** -0.5, 0.0234375, ((0, 2), (1, 64))),
        "child_omega": centred(keys[1], (N_CHILD, ORDER, SAMPLES), 1.0, 6.0, ((0, 2), (1, 64))),
        "parent_block": centred(keys[2], (PARENT_ROWS, BLOCK), BLOCK ** -0.5, 0.5, ((0, 128),)),
        "parent_omega": centred(keys[3], (PARENT_ROWS, SAMPLES), 1.0, 6.0, ((0, 128),)),
        "child_map": draw_child_map(jax.random.fold_in(keys[6], 71), 0),
        "leaf_order": draw_leaf_order(jax.random.fold_in(keys[6], 71), 0),
    }


def reference(front_update, child_omega, parent_block, parent_omega, child_map, leaf_order):
    assembled = jnp.zeros((PARENT_ROWS, SAMPLES), jnp.float32)
    for front_id in range(N_CHILD):
        sampled = jnp.dot(front_update[front_id], child_omega[front_id], preferred_element_type=jnp.float32)
        assembled = assembled.at[child_map[front_id]].add(sampled)
    leaf_blocks = PARENT_ROWS // BLOCK
    own_samples = jnp.einsum(
        "bij,bjr->bir",
        parent_block.reshape(leaf_blocks, BLOCK, BLOCK).astype(jnp.float32),
        parent_omega.reshape(leaf_blocks, BLOCK, SAMPLES).astype(jnp.float32),
        precision=lax.Precision.HIGHEST,
    ).reshape(PARENT_ROWS, SAMPLES)
    assembled = assembled + own_samples
    return assembled[leaf_order]
```

```python
import jax
import jax.numpy as jnp
from jax import lax
from jax.sharding import PartitionSpec as P


def split_up(value, dim, length):
    before, after = (value.shape[:dim], value.shape[dim + 1 :])
    return jnp.moveaxis(value.reshape(*before, length, -1, *after), dim, 0)


def in_order(blocks, dim):
    blocks = jnp.moveaxis(blocks, 0, dim)
    lengths = blocks.shape
    return blocks.reshape(*lengths[:dim], lengths[dim] * lengths[dim + 1], *lengths[dim + 2 :])


def one_exchange(value, axis, axes, splits, concats):
    sizes = [lax.axis_size(a) for a in axes]
    blocks = split_up(value, splits[0], sizes[0])
    blocks = jnp.moveaxis(split_up(blocks, splits[1] + 1, sizes[1]), 0, 1)
    inside = blocks.shape[2:]
    blocks = blocks.reshape(-1, *inside)
    blocks = lax.all_to_all(blocks, axis, split_axis=0, concat_axis=0, tiled=True)
    blocks = in_order(blocks.reshape(*sizes, *inside), concats[0] + 1)
    return in_order(blocks, concats[1])


def bucket_rank(owner_ids, owners):
    one_hot = (owner_ids[:, None] == jnp.arange(owners, dtype=jnp.int32)[None, :]).astype(jnp.int32)
    running = jnp.cumsum(one_hot, axis=0)
    return jnp.sum(one_hot * running, axis=1) - 1


def select_rows(targets, total, values):
    picker = (targets[None, :] == jnp.arange(total, dtype=jnp.int32)[:, None]).astype(jnp.float32)
    return jnp.dot(
        picker, values, precision=lax.Precision.HIGHEST, preferred_element_type=jnp.float32
    )


def pick_rows(sources, values):
    picker = (sources[:, None] == jnp.arange(values.shape[0], dtype=jnp.int32)[None, :]).astype(
        jnp.float32
    )
    return jnp.dot(
        picker, values, precision=lax.Precision.HIGHEST, preferred_element_type=jnp.float32
    )


def ranked(marked, values, capacity, empty):
    length = marked.shape[1]
    upto = jnp.tril(jnp.ones((length, length), jnp.bfloat16)).T
    rank = jnp.dot(marked.astype(jnp.bfloat16), upto, preferred_element_type=jnp.float32)
    rank = jnp.where(marked, rank.astype(jnp.int32), 0)
    kept = [
        jnp.sum(jnp.where(rank == k + 1, values - empty, 0), axis=1) + empty for k in range(capacity)
    ]
    return jnp.stack(kept, axis=1)


def body(front_update, child_omega, parent_block, parent_omega, child_map, leaf_order):
    children = lax.axis_size("child")
    row_count = lax.axis_size("rows")
    owners = children * row_count
    device_id = lax.axis_index("child") * row_count + lax.axis_index("rows")
    slab_rows = front_update[0]
    local_rows = slab_rows.shape[0]
    sample_cols = child_omega.shape[2]
    sampled = jnp.dot(
        slab_rows,
        lax.all_gather(child_omega, "rows", axis=1, tiled=True)[0],
        preferred_element_type=jnp.float32,
    )
    parent_dev = parent_block.shape[0]
    capacity = 2 * local_rows // owners
    route_table = child_map.reshape(owners, local_rows)
    my_targets = lax.dynamic_index_in_dim(route_table, device_id, 0, keepdims=False)
    target_owner = my_targets // parent_dev
    target_slot = target_owner * capacity + bucket_rank(target_owner, owners)
    outgoing = select_rows(target_slot, owners * capacity, sampled)
    incoming = one_exchange(
        outgoing.reshape(children, row_count, capacity, sample_cols),
        ("child", "rows"),
        ("child", "rows"),
        (0, 1),
        (0, 1),
    )
    incoming = incoming.reshape(owners * capacity, sample_cols)
    arrives = route_table // parent_dev == device_id
    places = ranked(arrives, route_table % parent_dev, capacity, parent_dev)
    assembled = select_rows(places.reshape(-1), parent_dev, incoming)
    leaf_size = parent_block.shape[1]
    leaf_blocks = parent_dev // leaf_size
    own_samples = jnp.einsum(
        "bij,bjr->bir",
        parent_block.reshape(leaf_blocks, leaf_size, leaf_size),
        parent_omega.reshape(leaf_blocks, leaf_size, sample_cols),
        preferred_element_type=jnp.float32,
    ).reshape(parent_dev, sample_cols)
    assembled = assembled + own_samples
    leaf_capacity = parent_dev // owners
    leaf_table = leaf_order.reshape(owners, parent_dev)
    leaving = ranked(leaf_table // parent_dev == device_id, leaf_table % parent_dev, leaf_capacity, 0)
    sending = pick_rows(leaving.reshape(-1), assembled)
    arrived = lax.all_to_all(
        sending.reshape(owners, leaf_capacity, sample_cols),
        ("child", "rows"),
        split_axis=0,
        concat_axis=0,
        tiled=True,
    )
    arrived = arrived.reshape(owners * leaf_capacity, sample_cols)
    natural = lax.dynamic_slice_in_dim(leaf_order, device_id * parent_dev, parent_dev)
    anchor = natural // parent_dev
    same_anchor = anchor[:, None] == anchor[None, :]
    place = jnp.arange(parent_dev, dtype=jnp.int32)
    earlier = place[None, :] < place[:, None]
    arrival_rank = jnp.sum((same_anchor & earlier).astype(jnp.int32), axis=1)
    return pick_rows(anchor * leaf_capacity + arrival_rank, arrived)


def solution(mesh):
    placed = (
        P("child", "rows", None),
        P("child", "rows", None),
        P(("child", "rows"), None),
        P(("child", "rows"), None),
        P(),
        P(),
    )
    return jax.shard_map(
        body, mesh=mesh, in_specs=placed, out_specs=P(("child", "rows"), None), check_vma=False
    )
```

```python
import functools

import jax
import jax.numpy as jnp
from jax import lax
from jax.experimental import pallas as pl
from jax.experimental.pallas import tpu as pltpu
from jax.sharding import PartitionSpec as P

MESH = pl.DeviceIdType.MESH
SIDE = 4
CHIPS = SIDE**3
OWNERS = 2 * CHIPS
SHARD = 960
PIECE = 160
PAIR = 2 * SHARD
CAP = 3
TILE = 8
WINDOW = 4
ORDERS = ((0, 1, 2), (1, 2, 0), (2, 0, 1))
BATCHES = (
    (0, 3, 3, 0, 0),
    (1, 3, 1, 0, 0),
    (1, 3, 1, 0, 1),
    (1, 3, 1, 0, 2),
    (0, 3, 1, 0, 3),
    (0, 1, 3, 3, 0),
    (1, 3, 1, 0, 3),
    (1, 1, 3, 3, 0),
    (0, 1, 1, 3, 3),
    (1, 1, 1, 3, 3),
)
WALK = (0, 1, 3, 2)


def moved(offset, dim, by):
    new = list(offset)
    new[dim] = (new[dim] + by) % SIDE
    return tuple(new)


def all_sends():
    sends = {(d, sign): [] for d in range(3) for sign in (1, -1)}
    for part, order in enumerate(ORDERS):
        for half, turn in enumerate((1, -1)):
            for phase in range(3):
                here = order[phase]
                for a in WALK:
                    for b in WALK:
                        inner = (a, b)
                        if any(inner[i] for i in range(2) if i >= phase):
                            continue
                        offset = [0, 0, 0]
                        for i in range(phase):
                            offset[order[i]] = inner[i]
                        for sign in (1, -1):
                            sends[here, sign].append((phase, 0, WALK.index(b), WALK.index(a), half, tuple(offset), part))
                        offset[here] = turn % SIDE
                        sends[here, turn].append((phase, 1, WALK.index(b), WALK.index(a), half, tuple(offset), part))
    return {link: sorted(found) for link, found in sends.items()}


def make_schedule(window):
    waiting = all_sends()
    links = list(waiting)
    arrived = {((0, 0, 0), part, half): -window for part in range(3) for half in range(2)}
    slots = []
    while any(waiting.values()):
        now, came = [], []
        for link in links:
            ready = [s for s in waiting[link] if arrived.get((s[5], s[6], s[4]), 10**6) + window <= len(slots)]
            assert ready
            chosen = ready[0]
            waiting[link].remove(chosen)
            now.append((link, chosen[5], chosen[6], chosen[4]))
            came.append((moved(chosen[5], *link), chosen[6], chosen[4]))
        for key in came:
            assert key not in arrived
            arrived[key] = len(slots)
        slots.append(now)
    return slots, arrived


def batch_members(batch):
    other, ny, nz, y0, z0 = batch
    return [(other, WALK[y0 + i % ny], WALK[z0 + i // ny]) for i in range(ny * nz)]


def ready_slot(batch, arrived):
    latest = 0
    for other, ry, rz in batch_members(batch):
        for rx in ((2, 1, 3) if other else (0, 1, 3)):
            for part in range(3):
                for half in range(2):
                    latest = max(latest, arrived[(rx, ry, rz), part, half])
    return latest


def two_parts(values):
    high = values.astype(jnp.bfloat16)
    low = (values - high.astype(jnp.float32)).astype(jnp.bfloat16)
    return jnp.concatenate([high, low], axis=-1)


def picked(picker, parts):
    both = jnp.dot(picker, parts, preferred_element_type=jnp.float32)
    return both[:, :128] + both[:, 128:]


def kernel(
    front, omega, block, parent_omega, t1, t2, t3, t4, out,
    gathered, slab, total, stacked, parts, send1, recv1, send2, recv2, p1, p2, p3, p4,
    own_sem, slab_sem, sent_sem, slot_sem, mate_sem, sent1, came1, sent2, came2,
):
    child = lax.axis_index("child")
    chip = lax.axis_index("rows")
    me = child * CHIPS + chip
    place = (lax.rem(chip, SIDE), lax.rem(chip // SIDE, SIDE), chip // (SIDE * SIDE))
    back = [[lax.rem(place[d] + SIDE - r, SIDE) for r in range(SIDE)] for d in range(3)]

    def chip_at(xyz):
        return xyz[2] * (SIDE * SIDE) + xyz[1] * SIDE + xyz[0]

    def source(offset):
        return chip_at([back[d][offset[d]] for d in range(3)])

    neighbour = {}
    for d in range(3):
        for sign in (1, -1):
            offset = [0, 0, 0]
            offset[d] = -sign % SIDE
            neighbour[d, sign] = source(offset)

    own = pltpu.make_async_copy(omega.at[0], gathered.at[pl.ds(chip * SHARD, SHARD)], own_sem)
    own.start()
    barrier = pltpu.get_barrier_semaphore()
    for there in neighbour.values():
        pl.semaphore_signal(barrier, inc=1, device_id=(child, there), device_id_type=MESH)
    pl.semaphore_signal(barrier, inc=1, device_id=(1 - child, chip), device_id_type=MESH)

    def walk(i):
        return i + i // 2 - 2 * (i // 3)

    def pair_of(batch, i):
        other, ny, nz, y0, z0 = batch
        y = lax.rem(place[1] + SIDE - walk(y0 + lax.rem(i, ny)), SIDE)
        z = lax.rem(place[2] + SIDE - walk(z0 + i // ny), SIDE)
        half = place[0] // 2
        half = 1 - half if other else half
        return (z * SIDE + y) * 2 + half

    def slab_copy(batch, first, i):
        columns = pl.ds(pl.multiple_of(pair_of(batch, i) * PAIR, PAIR), PAIR)
        return pltpu.make_async_copy(front.at[0, :, columns], slab.at[first + i], slab_sem.at[first + i])

    firsts, count = [], 0
    for batch in BATCHES:
        firsts.append(count)

        def start(i, carry, batch=batch, first=count):
            slab_copy(batch, first, i).start()
            return carry

        lax.fori_loop(0, batch[1] * batch[2], start, 0)
        count += batch[1] * batch[2]

    total[...] = jnp.zeros_like(total)
    own.wait()
    pl.semaphore_wait(barrier, 7)

    def piece(offset, part, half):
        return gathered.at[pl.ds(source(offset) * SHARD + part * (2 * PIECE) + half * PIECE, PIECE)]

    def wait_slot(t):
        rows = gathered.at[pl.ds(0, 6 * PIECE)]
        pltpu.make_async_remote_copy(
            rows, rows, sent_sem, slot_sem.at[t], device_id=(child, neighbour[0, 1]), device_id_type=MESH
        ).wait_recv()

    def multiply(number):
        batch, first = BATCHES[number], firsts[number]

        def one(i, carry):
            slab_copy(batch, first, i).wait()
            rows = pl.ds(pl.multiple_of(pair_of(batch, i) * PAIR, PAIR), PAIR)
            total[...] += jnp.dot(slab[first + i], gathered[rows, :], preferred_element_type=jnp.float32)
            return carry

        lax.fori_loop(0, batch[1] * batch[2], one, 0)

    def build(picker, length, column):
        def some(i, carry):
            rows = pl.ds(pl.multiple_of(i * 64, 64), 64)
            picker[rows, :] = jnp.where(column(rows, i), 1.0, 0.0).astype(jnp.bfloat16)
            return carry

        lax.fori_loop(0, length // 64, some, 0)

    def by_column(picker, table):
        width = picker.shape[1]
        build(
            picker,
            picker.shape[0],
            lambda rows, i: table[rows, :] == lax.broadcasted_iota(jnp.int32, (64, width), 1),
        )

    def by_row(picker, table):
        width = picker.shape[1]
        build(
            picker,
            picker.shape[0],
            lambda rows, i: table[...] == lax.broadcasted_iota(jnp.int32, (64, width), 0) + i * 64,
        )

    def own_rows():
        leaf = block.shape[1]
        rows = block.shape[0]
        for b in range(rows // leaf):
            value = jnp.dot(
                block[b * leaf : (b + 1) * leaf, :],
                parent_omega[b * leaf : (b + 1) * leaf, :],
                preferred_element_type=jnp.float32,
            )
            stacked[b * leaf : (b + 1) * leaf, :] = value[:, :128]
            stacked[rows + b * leaf : rows + (b + 1) * leaf, :] = value[:, 128:]

    slots, arrived = make_schedule(WINDOW)
    ready = [ready_slot(batch, arrived) for batch in BATCHES]
    done = 0
    for t in range(len(slots) + WINDOW):
        if t >= WINDOW:
            wait_slot(t - WINDOW)
        if t < len(slots):
            for link, offset, part, half in slots[t]:
                data = piece(offset, part, half)
                pltpu.make_async_remote_copy(
                    data, data, sent_sem, slot_sem.at[t], device_id=(child, neighbour[link]), device_id_type=MESH
                ).start()
        if t == 6:
            by_column(p1, t1)
        if t == 8:
            by_row(p2, t2)
        if t == 10:
            by_column(p3, t3)
        if t == 12:
            by_column(p4, t4)
        if t == 14:
            own_rows()
        while done < len(BATCHES) and ready[done] <= t - WINDOW:
            multiply(done)
            done += 1

    sent = gathered.at[pl.ds(0, 6 * PIECE * len(slots))]
    pltpu.make_async_remote_copy(
        sent, sent, sent_sem, slot_sem.at[0], device_id=(child, neighbour[0, 1]), device_id_type=MESH
    ).wait_send()

    pl.semaphore_signal(mate_sem, inc=1, device_id=(1 - child, chip), device_id_type=MESH)

    def fill(send, picker, height):
        def some(i, carry):
            rows = pl.ds(pl.multiple_of(i * 128, 128), 128)
            tiles = picked(picker[rows, :], parts[pl.ds(0, height), :]).reshape(128 // TILE, TILE, 128)
            send[pl.ds(pl.multiple_of(i * (128 // TILE), 128 // TILE), 128 // TILE)] = tiles
            return carry

        lax.fori_loop(0, OWNERS * TILE // 128, some, 0)

    def exchange(send, recv, sent_sem, came_sem):
        def one(step, carry):
            there = lax.rem(me + step, OWNERS)
            pltpu.make_async_remote_copy(
                send.at[there],
                recv.at[me],
                sent_sem,
                came_sem,
                device_id=(there // CHIPS, lax.rem(there, CHIPS)),
                device_id_type=MESH,
            ).start()
            return carry

        lax.fori_loop(1, OWNERS, one, 0)
        recv[me] = send[me]
        most = pl.ds(0, OWNERS - 1)
        everything = pltpu.make_async_remote_copy(
            send.at[most], recv.at[most], sent_sem, came_sem, device_id=(child, neighbour[0, 1]), device_id_type=MESH
        )
        everything.wait_recv()
        everything.wait_send()

    height = total.shape[0]
    parts[pl.ds(0, height), :] = two_parts(total[:, :128])
    parts[pl.ds(height, height), :] = two_parts(total[:, 128:])
    fill(send1, p1, 2 * height)
    pl.semaphore_wait(mate_sem, 1)
    exchange(send1, recv1, sent1, came1)
    parts[...] = two_parts(recv1[...].reshape(OWNERS * TILE, 128))
    rows = stacked.shape[0]

    def assemble(i, carry):
        some = pl.ds(pl.multiple_of(i * 128, 128), 128)
        stacked[some, :] += picked(p2[some, :], parts[...])
        return carry

    lax.fori_loop(0, rows // 128, assemble, 0)
    parts[pl.ds(0, rows), :] = two_parts(stacked[...])
    fill(send2, p3, rows)
    exchange(send2, recv2, sent2, came2)
    parts[...] = two_parts(recv2[...].reshape(OWNERS * TILE, 128))
    half = rows // 2
    for side in range(2):

        def finish(i, carry, side=side):
            some = pl.ds(pl.multiple_of(side * half + i * 128, 128), 128)
            out[pl.ds(pl.multiple_of(i * 128, 128), 128), side * 128 : (side + 1) * 128] = picked(p4[some, :], parts[...])
            return carry

        lax.fori_loop(0, half // 128, finish, 0)


def ranked(marked, values, capacity, empty):
    length = marked.shape[1]
    upto = jnp.tril(jnp.ones((length, length), jnp.bfloat16)).T
    rank = jnp.dot(marked.astype(jnp.bfloat16), upto, preferred_element_type=jnp.float32)
    rank = jnp.where(marked, rank.astype(jnp.int32), 0)
    kept = [
        jnp.sum(jnp.where(rank == k + 1, values - empty, 0), axis=1) + empty for k in range(capacity)
    ]
    return jnp.stack(kept, axis=1)


def both_halves(table, shift):
    other = jnp.where(table < 0, -1, table + shift)
    return jnp.concatenate([table, other, jnp.full((table.shape[0], 2), -1, jnp.int32)], axis=1)


def body(front_update, child_omega, parent_block, parent_omega, child_map, leaf_order):
    device_id = lax.axis_index("child") * CHIPS + lax.axis_index("rows")
    local_rows = front_update.shape[1]
    sample_cols = child_omega.shape[2]
    parent_dev = parent_block.shape[0]
    route = child_map.reshape(OWNERS, local_rows)
    mine = lax.dynamic_index_in_dim(route, device_id, 0, keepdims=False) // parent_dev
    to_owner = mine[None, :] == jnp.arange(OWNERS, dtype=jnp.int32)[:, None]
    t1 = ranked(to_owner, jnp.arange(local_rows, dtype=jnp.int32)[None, :], CAP, -1)
    t1 = both_halves(t1, local_rows).reshape(OWNERS * TILE, 1)
    t2 = ranked(route // parent_dev == device_id, route % parent_dev, CAP, -1)
    t2 = both_halves(t2, parent_dev).reshape(1, OWNERS * TILE)
    leaves = leaf_order.reshape(OWNERS, parent_dev)
    t3 = ranked(leaves // parent_dev == device_id, leaves % parent_dev, CAP, -1)
    t3 = both_halves(t3, parent_dev).reshape(OWNERS * TILE, 1)
    anchor = lax.dynamic_index_in_dim(leaves, device_id, 0, keepdims=False) // parent_dev
    where = jnp.arange(parent_dev, dtype=jnp.int32)
    before = (anchor[:, None] == anchor[None, :]) & (where[None, :] < where[:, None])
    t4 = anchor * TILE + jnp.sum(before.astype(jnp.int32), axis=1)
    t4 = jnp.concatenate([t4, t4 + CAP]).reshape(2 * parent_dev, 1)

    slots, _ = make_schedule(WINDOW)
    vmem = pl.BlockSpec(memory_space=pltpu.VMEM)
    anywhere = pl.BlockSpec(memory_space=pl.ANY)
    tiles = pltpu.VMEM((OWNERS, TILE, 128), jnp.float32)
    slot_rows = OWNERS * TILE
    dma = pltpu.SemaphoreType.DMA
    return pl.pallas_call(
        kernel,
        out_shape=jax.ShapeDtypeStruct((parent_dev, sample_cols), jnp.float32),
        in_specs=[anywhere, anywhere, vmem, vmem, vmem, vmem, vmem, vmem],
        out_specs=vmem,
        scratch_shapes=[
            pltpu.VMEM((CHIPS * SHARD, sample_cols), jnp.bfloat16),
            pltpu.VMEM((CHIPS // 2, local_rows, PAIR), jnp.bfloat16),
            pltpu.VMEM((local_rows, sample_cols), jnp.float32),
            pltpu.VMEM((2 * parent_dev, 128), jnp.float32),
            pltpu.VMEM((slot_rows, 256), jnp.bfloat16),
            tiles,
            tiles,
            tiles,
            tiles,
            pltpu.VMEM((slot_rows, 2 * local_rows), jnp.bfloat16),
            pltpu.VMEM((2 * parent_dev, slot_rows), jnp.bfloat16),
            pltpu.VMEM((slot_rows, 2 * parent_dev), jnp.bfloat16),
            pltpu.VMEM((2 * parent_dev, slot_rows), jnp.bfloat16),
            dma,
            dma((CHIPS // 2,)),
            dma,
            dma((len(slots),)),
            pltpu.SemaphoreType.REGULAR,
            dma,
            dma,
            dma,
            dma,
        ],
        compiler_params=pltpu.CompilerParams(
            collective_id=0, has_side_effects=True, vmem_limit_bytes=67043328
        ),
    )(front_update, child_omega, parent_block, parent_omega, t1, t2, t3, t4)


def solution(mesh):
    placed = (
        P("child", "rows", None),
        P("child", "rows", None),
        P(("child", "rows"), None),
        P(("child", "rows"), None),
        P(),
        P(),
    )
    return jax.shard_map(
        body, mesh=mesh, in_specs=placed, out_specs=P(("child", "rows"), None), check_vma=False
    )
```

```python
import functools

import jax
import jax.numpy as jnp
from jax import lax
from jax.experimental import pallas as pl
from jax.experimental.pallas import tpu as pltpu
from jax.sharding import PartitionSpec as P

MESH = pl.DeviceIdType.MESH
SIDE = 4
CHIPS = SIDE**3
OWNERS = 2 * CHIPS
SHARD = 960
PIECE = 160
PAIR = 2 * SHARD
CAP = 3
TILE = 8
WINDOW = 4
ORDERS = ((0, 1, 2), (1, 2, 0), (2, 0, 1))
BATCHES = (
    (0, 3, 3, 0, 0),
    (1, 3, 1, 0, 0),
    (1, 3, 1, 0, 1),
    (1, 3, 1, 0, 2),
    (0, 3, 1, 0, 3),
    (0, 1, 3, 3, 0),
    (1, 3, 1, 0, 3),
    (1, 1, 3, 3, 0),
    (0, 1, 1, 3, 3),
    (1, 1, 1, 3, 3),
)
WALK = (0, 1, 3, 2)


def moved(offset, dim, by):
    new = list(offset)
    new[dim] = (new[dim] + by) % SIDE
    return tuple(new)


def all_sends():
    sends = {(d, sign): [] for d in range(3) for sign in (1, -1)}
    for part, order in enumerate(ORDERS):
        for half, turn in enumerate((1, -1)):
            for phase in range(3):
                here = order[phase]
                for a in WALK:
                    for b in WALK:
                        inner = (a, b)
                        if any(inner[i] for i in range(2) if i >= phase):
                            continue
                        offset = [0, 0, 0]
                        for i in range(phase):
                            offset[order[i]] = inner[i]
                        for sign in (1, -1):
                            sends[here, sign].append((phase, 0, WALK.index(b), WALK.index(a), half, tuple(offset), part))
                        offset[here] = turn % SIDE
                        sends[here, turn].append((phase, 1, WALK.index(b), WALK.index(a), half, tuple(offset), part))
    return {link: sorted(found) for link, found in sends.items()}


def make_schedule(window):
    waiting = all_sends()
    links = list(waiting)
    arrived = {((0, 0, 0), part, half): -window for part in range(3) for half in range(2)}
    slots = []
    while any(waiting.values()):
        now, came = [], []
        for link in links:
            ready = [s for s in waiting[link] if arrived.get((s[5], s[6], s[4]), 10**6) + window <= len(slots)]
            assert ready
            chosen = ready[0]
            waiting[link].remove(chosen)
            now.append((link, chosen[5], chosen[6], chosen[4]))
            came.append((moved(chosen[5], *link), chosen[6], chosen[4]))
        for key in came:
            assert key not in arrived
            arrived[key] = len(slots)
        slots.append(now)
    return slots, arrived


def batch_members(batch):
    other, ny, nz, y0, z0 = batch
    return [(other, WALK[y0 + i % ny], WALK[z0 + i // ny]) for i in range(ny * nz)]


def ready_slot(batch, arrived):
    latest = 0
    for other, ry, rz in batch_members(batch):
        for rx in ((2, 1, 3) if other else (0, 1, 3)):
            for part in range(3):
                for half in range(2):
                    latest = max(latest, arrived[(rx, ry, rz), part, half])
    return latest


def two_parts(values):
    high = values.astype(jnp.bfloat16)
    low = (values - high.astype(jnp.float32)).astype(jnp.bfloat16)
    return jnp.concatenate([high, low], axis=-1)


def picked(picker, parts):
    both = jnp.dot(picker, parts, preferred_element_type=jnp.float32)
    return both[:, :128] + both[:, 128:]


def kernel(
    front, omega, block_in, parent_in, child_map, leaf_order, out_rows,
    gathered, slab, total, stacked, parts, send1, recv1, send2, recv2, p1, p2, p3, p4,
    block, parent_omega, map_rows, leaf_rows, map_table, columns, scratch,
    own_sem, slab_sem, in_sem, sent_sem, slot_sem, mate_sem, sent1, came1, sent2, came2,
):
    child = lax.axis_index("child")
    chip = lax.axis_index("rows")
    me = child * CHIPS + chip
    place = (lax.rem(chip, SIDE), lax.rem(chip // SIDE, SIDE), chip // (SIDE * SIDE))
    back = [[lax.rem(place[d] + SIDE - r, SIDE) for r in range(SIDE)] for d in range(3)]
    height = total.shape[0]
    rows = block.shape[0]

    def chip_at(xyz):
        return xyz[2] * (SIDE * SIDE) + xyz[1] * SIDE + xyz[0]

    def source(offset):
        return chip_at([back[d][offset[d]] for d in range(3)])

    neighbour = {}
    for d in range(3):
        for sign in (1, -1):
            offset = [0, 0, 0]
            offset[d] = -sign % SIDE
            neighbour[d, sign] = source(offset)

    own = pltpu.make_async_copy(omega.at[0], gathered.at[pl.ds(chip * SHARD, SHARD)], own_sem)
    own.start()
    barrier = pltpu.get_barrier_semaphore()
    for there in neighbour.values():
        pl.semaphore_signal(barrier, inc=1, device_id=(child, there), device_id_type=MESH)
    pl.semaphore_signal(barrier, inc=1, device_id=(1 - child, chip), device_id_type=MESH)

    def walk(i):
        return i + i // 2 - 2 * (i // 3)

    def pair_of(batch, i):
        other, ny, nz, y0, z0 = batch
        y = lax.rem(place[1] + SIDE - walk(y0 + lax.rem(i, ny)), SIDE)
        z = lax.rem(place[2] + SIDE - walk(z0 + i // ny), SIDE)
        half = place[0] // 2
        half = 1 - half if other else half
        return (z * SIDE + y) * 2 + half

    def slab_copy(batch, first, i):
        columns = pl.ds(pl.multiple_of(pair_of(batch, i) * PAIR, PAIR), PAIR)
        return pltpu.make_async_copy(front.at[0, :, columns], slab.at[first + i], slab_sem.at[first + i])

    firsts, count = [], 0
    for batch in BATCHES:
        firsts.append(count)
        count += batch[1] * batch[2]
    inputs = [
        pltpu.make_async_copy(source_ref, kept, in_sem.at[i])
        for i, (source_ref, kept) in enumerate(
            ((child_map, map_rows), (leaf_order, leaf_rows), (block_in, block), (parent_in, parent_omega))
        )
    ]

    def start_loads():
        for copy in inputs:
            copy.start()
        for batch, first in zip(BATCHES, firsts):

            def start(i, carry, batch=batch, first=first):
                slab_copy(batch, first, i).start()
                return carry

            lax.fori_loop(0, batch[1] * batch[2], start, 0)
        total[...] = jnp.zeros_like(total)

    def piece(offset, part, half):
        return gathered.at[pl.ds(source(offset) * SHARD + part * (2 * PIECE) + half * PIECE, PIECE)]

    def wait_slot(t):
        some = gathered.at[pl.ds(0, 6 * PIECE)]
        pltpu.make_async_remote_copy(
            some, some, sent_sem, slot_sem.at[t], device_id=(child, neighbour[0, 1]), device_id_type=MESH
        ).wait_recv()

    def multiply(number):
        batch, first = BATCHES[number], firsts[number]

        def one(i, carry):
            slab_copy(batch, first, i).wait()
            some = pl.ds(pl.multiple_of(pair_of(batch, i) * PAIR, PAIR), PAIR)
            total[...] += jnp.dot(slab[first + i], gathered[some, :], preferred_element_type=jnp.float32)
            return carry

        lax.fori_loop(0, batch[1] * batch[2], one, 0)

    def clear():
        recv1[...] = jnp.zeros_like(recv1)
        recv2[...] = jnp.zeros_like(recv2)

    def map_in():
        inputs[0].wait()
        for u in range(CHIPS // 2):
            for c in range(2):
                map_table[c * (CHIPS // 2) + u : c * (CHIPS // 2) + u + 1, :] = map_rows[
                    c : c + 1, u * 2 * height : (u + 1) * 2 * height
                ]

    def iota(shape, dim):
        return lax.broadcasted_iota(jnp.int32, shape, dim)

    def upto(n, segment):
        i, j = iota((n, n), 0), iota((n, n), 1)
        same = i <= j
        if segment < n:
            same = same & ((i >= segment) == (j >= segment))
        return jnp.where(same, 1.0, 0.0).astype(jnp.bfloat16)

    def prefix(marked, segment):
        ones = jnp.where(marked, 1.0, 0.0).astype(jnp.bfloat16)
        return jnp.dot(ones, upto(marked.shape[1], segment), preferred_element_type=jnp.float32)

    def find_places(values, segment):
        low = me * rows
        marked = (values >= low) & (values < low + rows)
        rank = prefix(marked, segment)
        local = (values - low + 1).astype(jnp.float32)
        n = values.shape[1]
        lane = iota(values.shape, 1)
        for e in range(n // segment):
            inside = marked & (lane >= e * segment) & (lane < (e + 1) * segment)
            for k in range(CAP):
                found = jnp.sum(jnp.where(inside & (rank == k + 1.0), local, 0.0), axis=1, keepdims=True) - 1.0
                columns[e * CAP + k, 0 : values.shape[0], :] = jnp.broadcast_to(found, (values.shape[0], 128))

    def place_rows(group, segments, width):
        def one(b, carry):
            index = group * 16 + b
            row = index // segments
            j = iota((TILE, 128), 0)
            lane = iota((TILE, 128), 1).astype(jnp.float32)
            kept = jnp.full((TILE, 128), -1.0, jnp.float32)
            for k in range(CAP):
                if segments == 1:
                    at = columns[k, pl.ds(row, 1), :]
                else:
                    odd = jnp.full((1, 128), lax.rem(index, 2), jnp.int32)
                    at = jnp.where(odd == 0, columns[k, pl.ds(row, 1), :], columns[CAP + k, pl.ds(row, 1), :])
                at = jnp.broadcast_to(at, (TILE, 128))
                kept = jnp.where(j == k, at, kept)
                shifted = at if width == rows else jnp.where(at < 0.0, -1.0, at + float(rows))
                kept = jnp.where(j == CAP + k, shifted, kept)
            for t in range(width // 128):
                scratch[pl.ds(pl.multiple_of(b * TILE, TILE), TILE), t * 128 : (t + 1) * 128] = jnp.where(
                    kept == lane + float(t * 128), 1.0, 0.0
                )
            return carry

        lax.fori_loop(0, 16, one, 0)

    def turn(picker, group):
        for t in range(2 * rows // 128):
            picker[t * 128 : (t + 1) * 128, pl.ds(pl.multiple_of(group * 128, 128), 128)] = jnp.transpose(
                scratch[:, t * 128 : (t + 1) * 128]
            ).astype(jnp.bfloat16)

    def over_groups(step):
        def one(group, carry):
            step(group)
            return carry

        return [lambda first=first: lax.fori_loop(first, first + 2, one, 0) for first in range(0, 8, 2)]

    def p2_group(group):
        place_rows(group, 2, 2 * rows)
        turn(p2, group)

    def p3_group(group):
        place_rows(group, 1, rows)
        p3[pl.ds(pl.multiple_of(group * 128, 128), 128), :] = scratch[:, 0:rows].astype(jnp.bfloat16)

    def codes(values, segment):
        n = values.shape[1]
        owner = iota((OWNERS, n), 0)
        spread = jnp.broadcast_to(values, (OWNERS, n))
        marked = (spread >= owner * rows) & (spread < owner * rows + rows)
        rank = prefix(marked, segment)
        code = (owner * TILE).astype(jnp.float32) + rank - 1.0
        return jnp.sum(jnp.where(marked, code, 0.0), axis=0, keepdims=True)

    def p1_all():
        both = codes(map_table[pl.ds(child * (CHIPS // 2) + chip // 2, 1), :], height)
        odd = jnp.full((1, height), lax.rem(chip, 2), jnp.int32)
        code = jnp.where(odd == 0, both[:, 0:height], both[:, height : 2 * height])

        def some(i, carry):
            slot = iota((128, height), 0)
            j = slot & (TILE - 1)
            wanted = jnp.where(j < CAP, slot, jnp.where(j < 2 * CAP, slot - CAP, -(10**6))) + i * 128
            p1[pl.ds(pl.multiple_of(i * 128, 128), 128), :] = jnp.where(
                wanted.astype(jnp.float32) == jnp.broadcast_to(code, (128, height)), 1.0, 0.0
            ).astype(jnp.bfloat16)
            return carry

        lax.fori_loop(0, OWNERS * TILE // 128, some, 0)

    def p4_codes():
        mine = [leaf_rows[pl.ds(me * CAP + c, 1), :] for c in range(CAP)]
        code = codes(jnp.concatenate(mine, axis=1), rows)
        columns[0, 0:CAP, :] = jnp.concatenate([code[:, c * 128 : (c + 1) * 128] for c in range(CAP)], axis=0)

    def p4_group(group):
        for t in range(2 * CAP):
            code = jnp.broadcast_to(columns[0, t % CAP : t % CAP + 1, :], (128, 128))
            slot = (iota((128, 128), 0) + group * 128 - (t // CAP) * CAP).astype(jnp.float32)
            scratch[:, t * 128 : (t + 1) * 128] = jnp.where(slot == code, 1.0, 0.0)
        turn(p4, group)

    def leaf_places():
        inputs[1].wait()
        find_places(
            jnp.concatenate([leaf_rows[pl.ds(c, OWNERS, stride=CAP), :] for c in range(CAP)], axis=1), rows
        )

    def own_rows():
        inputs[2].wait()
        inputs[3].wait()
        leaf = block.shape[1]
        for b in range(rows // leaf):
            value = jnp.dot(
                block[b * leaf : (b + 1) * leaf, :],
                parent_omega[b * leaf : (b + 1) * leaf, :],
                preferred_element_type=jnp.float32,
            )
            stacked[b * leaf : (b + 1) * leaf, :] = value[:, :128]
            stacked[rows + b * leaf : rows + (b + 1) * leaf, :] = value[:, 128:]

    jobs = [start_loads, clear, map_in, lambda: find_places(map_table[...], height)]
    jobs += over_groups(p2_group)
    jobs += [p1_all, leaf_places]
    jobs += over_groups(p3_group)
    jobs += [p4_codes]
    jobs += over_groups(p4_group)
    jobs += [own_rows]

    own.wait()
    pl.semaphore_wait(barrier, 7)
    slots, arrived = make_schedule(WINDOW)
    ready = [ready_slot(batch, arrived) for batch in BATCHES]
    done = 0
    for t in range(len(slots) + WINDOW):
        if t >= WINDOW:
            wait_slot(t - WINDOW)
        if t < len(slots):
            for link, offset, part, half in slots[t]:
                data = piece(offset, part, half)
                pltpu.make_async_remote_copy(
                    data, data, sent_sem, slot_sem.at[t], device_id=(child, neighbour[link]), device_id_type=MESH
                ).start()
        if t >= WINDOW - 1 and jobs:
            jobs.pop(0)()
        if t == len(slots) + WINDOW - 1:
            pl.semaphore_signal(mate_sem, inc=1, device_id=(1 - child, chip), device_id_type=MESH)
        while done < len(BATCHES) and ready[done] <= t - WINDOW:
            multiply(done)
            done += 1

    def fill(send, picker, values):
        n = values.shape[1]

        def some(i, carry):
            both = jnp.dot(
                picker[pl.ds(pl.multiple_of(i * 512, 512), 512), :], values, preferred_element_type=jnp.float32
            )
            left = iota((512, 128), 0) & (TILE - 1)
            tile = jnp.where(left < CAP, both[:, 0:128] + both[:, 128:256], both[:, 256:384] + both[:, 384:512])
            send[pl.ds(pl.multiple_of(i * (512 // TILE), 512 // TILE), 512 // TILE)] = tile.reshape(512 // TILE, TILE, 128)
            return carry

        lax.fori_loop(0, OWNERS * TILE // 512, some, 0)

    used = pl.ds(0, 2 * CAP)

    def exchange(send, recv, sent_sem, came_sem):
        order = []
        for dx in range(SIDE):
            for dy in range(SIDE):
                for dz in range(SIDE):
                    for other in range(2):
                        far = sum(min(v, SIDE - v) for v in (dx, dy, dz))
                        if far or other:
                            order.append((-far, dx, dy, dz, other))
        for _, dx, dy, dz, other in sorted(order):
            to = source((dx, dy, dz))
            kid = 1 - child if other else child
            pltpu.make_async_remote_copy(
                send.at[kid * CHIPS + to, used],
                recv.at[me, used],
                sent_sem,
                came_sem,
                device_id=(kid, to),
                device_id_type=MESH,
            ).start()
        recv[me] = send[me]
        most = pl.ds(0, OWNERS - 1)
        everything = pltpu.make_async_remote_copy(
            send.at[most, used],
            recv.at[most, used],
            sent_sem,
            came_sem,
            device_id=(child, neighbour[0, 1]),
            device_id_type=MESH,
        )
        everything.wait_recv()
        return everything

    fill(send1, p1, jnp.concatenate([two_parts(total[:, :128]), two_parts(total[:, 128:])], axis=1))
    pl.semaphore_wait(mate_sem, 1)
    first = exchange(send1, recv1, sent1, came1)
    parts[...] = two_parts(recv1[...].reshape(OWNERS * TILE, 128))
    for side in range(2):
        stacked[side * rows : (side + 1) * rows, :] += picked(p2[side * rows : (side + 1) * rows, :], parts[...])
    fill(send2, p3, jnp.concatenate([two_parts(stacked[0:rows, :]), two_parts(stacked[rows : 2 * rows, :])], axis=1))
    second = exchange(send2, recv2, sent2, came2)
    parts[...] = two_parts(recv2[...].reshape(OWNERS * TILE, 128))
    for side in range(2):
        out_rows[:, side * 128 : (side + 1) * 128] = picked(p4[side * rows : (side + 1) * rows, :], parts[...])
    first.wait_send()
    second.wait_send()
    sent = gathered.at[pl.ds(0, 6 * PIECE * len(slots))]
    pltpu.make_async_remote_copy(
        sent, sent, sent_sem, slot_sem.at[0], device_id=(child, neighbour[0, 1]), device_id_type=MESH
    ).wait_send()


def body(front_update, child_omega, parent_block, parent_omega, child_map, leaf_order):
    local_rows = front_update.shape[1]
    sample_cols = child_omega.shape[2]
    parent_dev, leaf_size = parent_block.shape
    slots, _ = make_schedule(WINDOW)
    vmem = pl.BlockSpec(memory_space=pltpu.VMEM)
    anywhere = pl.BlockSpec(memory_space=pl.ANY)
    tiles = pltpu.VMEM((OWNERS, TILE, 128), jnp.float32)
    slot_rows = OWNERS * TILE
    dma = pltpu.SemaphoreType.DMA
    result = pl.pallas_call(
        kernel,
        out_shape=jax.ShapeDtypeStruct((parent_dev, sample_cols), jnp.float32),
        in_specs=[anywhere] * 6,
        out_specs=vmem,
        scratch_shapes=[
            pltpu.VMEM((CHIPS * SHARD, sample_cols), jnp.bfloat16),
            pltpu.VMEM((CHIPS // 2, local_rows, PAIR), jnp.bfloat16),
            pltpu.VMEM((local_rows, sample_cols), jnp.float32),
            pltpu.VMEM((2 * parent_dev, 128), jnp.float32),
            pltpu.VMEM((slot_rows, 256), jnp.bfloat16),
            tiles,
            tiles,
            tiles,
            tiles,
            pltpu.VMEM((slot_rows, local_rows), jnp.bfloat16),
            pltpu.VMEM((2 * parent_dev, slot_rows), jnp.bfloat16),
            pltpu.VMEM((slot_rows, parent_dev), jnp.bfloat16),
            pltpu.VMEM((2 * parent_dev, slot_rows), jnp.bfloat16),
            pltpu.VMEM((parent_dev, leaf_size), jnp.bfloat16),
            pltpu.VMEM((parent_dev, sample_cols), jnp.bfloat16),
            pltpu.VMEM(child_map.shape, jnp.int32),
            pltpu.VMEM((parent_dev, 128), jnp.int32),
            pltpu.VMEM((OWNERS // 2, 2 * local_rows), jnp.int32),
            pltpu.VMEM((2 * CAP, OWNERS, 128), jnp.float32),
            pltpu.VMEM((128, 2 * parent_dev), jnp.float32),
            dma,
            dma((CHIPS // 2,)),
            dma((4,)),
            dma,
            dma((len(slots),)),
            pltpu.SemaphoreType.REGULAR,
            dma,
            dma,
            dma,
            dma,
        ],
        compiler_params=pltpu.CompilerParams(
            collective_id=0, has_side_effects=True, vmem_limit_bytes=67043328
        ),
    )(front_update, child_omega, parent_block, parent_omega, child_map, leaf_order.reshape(parent_dev, 128))
    return result


def solution(mesh):
    placed = (
        P("child", "rows", None),
        P("child", "rows", None),
        P(("child", "rows"), None),
        P(("child", "rows"), None),
        P(),
        P(),
    )
    return jax.shard_map(
        body, mesh=mesh, in_specs=placed, out_specs=P(("child", "rows"), None), check_vma=False
    )
```

```python
import functools

import jax
import jax.numpy as jnp
from jax import lax
from jax.experimental import pallas as pl
from jax.experimental.pallas import tpu as pltpu
from jax.sharding import PartitionSpec as P

MESH = pl.DeviceIdType.MESH
SIDE = 4
CHIPS = SIDE**3
OWNERS = 2 * CHIPS
SHARD = 960
PIECE = 160
PAIR = 2 * SHARD
CAP = 3
TILE = 8
WINDOW = 4
ORDERS = ((0, 1, 2), (1, 2, 0), (2, 0, 1))
BATCHES = (
    (0, 3, 3, 0, 0),
    (1, 3, 1, 0, 0),
    (1, 3, 1, 0, 1),
    (1, 3, 1, 0, 2),
    (0, 3, 1, 0, 3),
    (0, 1, 3, 3, 0),
    (1, 2, 1, 0, 3),
    (1, 1, 2, 3, 0),
    (1, 1, 1, 2, 3),
    (1, 1, 1, 3, 2),
    (0, 1, 1, 3, 3),
    (1, 1, 1, 3, 3),
)
WALK = (0, 1, 3, 2)


def moved(offset, dim, by):
    new = list(offset)
    new[dim] = (new[dim] + by) % SIDE
    return tuple(new)


def all_sends():
    sends = {(d, sign): [] for d in range(3) for sign in (1, -1)}
    for part, order in enumerate(ORDERS):
        for half, turn in enumerate((1, -1)):
            for phase in range(3):
                here = order[phase]
                for a in WALK:
                    for b in WALK:
                        inner = (a, b)
                        if any(inner[i] for i in range(2) if i >= phase):
                            continue
                        offset = [0, 0, 0]
                        for i in range(phase):
                            offset[order[i]] = inner[i]
                        for sign in (1, -1):
                            sends[here, sign].append((phase, 0, WALK.index(b), WALK.index(a), half, tuple(offset), part))
                        offset[here] = turn % SIDE
                        sends[here, turn].append((phase, 1, WALK.index(b), WALK.index(a), half, tuple(offset), part))
    return {link: sorted(found) for link, found in sends.items()}


def make_schedule(window):
    waiting = all_sends()
    links = list(waiting)
    arrived = {((0, 0, 0), part, half): -window for part in range(3) for half in range(2)}
    slots = []
    while any(waiting.values()):
        now, came = [], []
        for link in links:
            ready = [s for s in waiting[link] if arrived.get((s[5], s[6], s[4]), 10**6) + window <= len(slots)]
            assert ready
            chosen = ready[0]
            waiting[link].remove(chosen)
            now.append((link, chosen[5], chosen[6], chosen[4]))
            came.append((moved(chosen[5], *link), chosen[6], chosen[4]))
        for key in came:
            assert key not in arrived
            arrived[key] = len(slots)
        slots.append(now)
    return slots, arrived


def batch_members(batch):
    other, ny, nz, y0, z0 = batch
    return [(other, WALK[y0 + i % ny], WALK[z0 + i // ny]) for i in range(ny * nz)]


def ready_slot(batch, arrived):
    latest = 0
    for other, ry, rz in batch_members(batch):
        for rx in ((2, 1, 3) if other else (0, 1, 3)):
            for part in range(3):
                for half in range(2):
                    latest = max(latest, arrived[(rx, ry, rz), part, half])
    return latest


def two_parts(values):
    high = values.astype(jnp.bfloat16)
    low = (values - high.astype(jnp.float32)).astype(jnp.bfloat16)
    return jnp.concatenate([high, low], axis=-1)


def picked(picker, parts):
    both = jnp.dot(picker, parts, preferred_element_type=jnp.float32)
    return both[:, :128] + both[:, 128:]


def kernel(
    front, omega, block_in, parent_in, child_map, leaf_order, out_rows,
    gathered, slab, total, stacked, parts, send1, recv1, send2, recv2, p1, p2, p3, p4,
    block, parent_omega, map_rows, leaf_rows, map_table, columns, scratch,
    own_sem, slab_sem, in_sem, sent_sem, slot_sem, mate_sem, sent1, came1, sent2, came2,
):
    child = lax.axis_index("child")
    chip = lax.axis_index("rows")
    me = child * CHIPS + chip
    place = (lax.rem(chip, SIDE), lax.rem(chip // SIDE, SIDE), chip // (SIDE * SIDE))
    back = [[lax.rem(place[d] + SIDE - r, SIDE) for r in range(SIDE)] for d in range(3)]
    height = total.shape[0]
    rows = block.shape[0]

    def chip_at(xyz):
        return xyz[2] * (SIDE * SIDE) + xyz[1] * SIDE + xyz[0]

    def source(offset):
        return chip_at([back[d][offset[d]] for d in range(3)])

    neighbour = {}
    for d in range(3):
        for sign in (1, -1):
            offset = [0, 0, 0]
            offset[d] = -sign % SIDE
            neighbour[d, sign] = source(offset)

    own = pltpu.make_async_copy(omega.at[0], gathered.at[pl.ds(chip * SHARD, SHARD)], own_sem)
    own.start()
    barrier = pltpu.get_barrier_semaphore()
    for there in neighbour.values():
        pl.semaphore_signal(barrier, inc=1, device_id=(child, there), device_id_type=MESH)
    pl.semaphore_signal(barrier, inc=1, device_id=(1 - child, chip), device_id_type=MESH)

    def walk(i):
        return i + i // 2 - 2 * (i // 3)

    def pair_of(batch, i):
        other, ny, nz, y0, z0 = batch
        y = lax.rem(place[1] + SIDE - walk(y0 + lax.rem(i, ny)), SIDE)
        z = lax.rem(place[2] + SIDE - walk(z0 + i // ny), SIDE)
        half = place[0] // 2
        half = 1 - half if other else half
        return (z * SIDE + y) * 2 + half

    def slab_copy(batch, first, i):
        columns = pl.ds(pl.multiple_of(pair_of(batch, i) * PAIR, PAIR), PAIR)
        return pltpu.make_async_copy(front.at[0, :, columns], slab.at[first + i], slab_sem.at[first + i])

    firsts, count = [], 0
    for batch in BATCHES:
        firsts.append(count)
        count += batch[1] * batch[2]
    inputs = [
        pltpu.make_async_copy(source_ref, kept, in_sem.at[i])
        for i, (source_ref, kept) in enumerate(
            ((child_map, map_rows), (leaf_order, leaf_rows), (block_in, block), (parent_in, parent_omega))
        )
    ]

    def start_loads():
        for copy in inputs:
            copy.start()
        for batch, first in zip(BATCHES, firsts):

            def start(i, carry, batch=batch, first=first):
                slab_copy(batch, first, i).start()
                return carry

            lax.fori_loop(0, batch[1] * batch[2], start, 0)
        total[...] = jnp.zeros_like(total)

    def piece(offset, part, half):
        return gathered.at[pl.ds(source(offset) * SHARD + part * (2 * PIECE) + half * PIECE, PIECE)]

    def wait_slot(t):
        some = gathered.at[pl.ds(0, 6 * PIECE)]
        pltpu.make_async_remote_copy(
            some, some, sent_sem, slot_sem.at[t], device_id=(child, neighbour[0, 1]), device_id_type=MESH
        ).wait_recv()

    def multiply(number):
        batch, first = BATCHES[number], firsts[number]

        def one(i, carry):
            slab_copy(batch, first, i).wait()
            some = pl.ds(pl.multiple_of(pair_of(batch, i) * PAIR, PAIR), PAIR)
            total[...] += jnp.dot(slab[first + i], gathered[some, :], preferred_element_type=jnp.float32)
            return carry

        lax.fori_loop(0, batch[1] * batch[2], one, 0)

    def clear():
        recv1[...] = jnp.zeros_like(recv1)
        recv2[...] = jnp.zeros_like(recv2)

    def map_in():
        inputs[0].wait()
        for u in range(CHIPS // 2):
            for c in range(2):
                map_table[c * (CHIPS // 2) + u : c * (CHIPS // 2) + u + 1, :] = map_rows[
                    c : c + 1, u * 2 * height : (u + 1) * 2 * height
                ]

    def iota(shape, dim):
        return lax.broadcasted_iota(jnp.int32, shape, dim)

    def upto(n, segment):
        i, j = iota((n, n), 0), iota((n, n), 1)
        same = i <= j
        if segment < n:
            same = same & ((i >= segment) == (j >= segment))
        return jnp.where(same, 1.0, 0.0).astype(jnp.bfloat16)

    def prefix(marked, segment):
        ones = jnp.where(marked, 1.0, 0.0).astype(jnp.bfloat16)
        return jnp.dot(ones, upto(marked.shape[1], segment), preferred_element_type=jnp.float32)

    def find_places(values, segment):
        low = me * rows
        marked = (values >= low) & (values < low + rows)
        rank = prefix(marked, segment)
        local = (values - low + 1).astype(jnp.float32)
        n = values.shape[1]
        lane = iota(values.shape, 1)
        for e in range(n // segment):
            inside = marked & (lane >= e * segment) & (lane < (e + 1) * segment)
            for k in range(CAP):
                found = jnp.sum(jnp.where(inside & (rank == k + 1.0), local, 0.0), axis=1, keepdims=True) - 1.0
                columns[e * CAP + k, 0 : values.shape[0], :] = jnp.broadcast_to(found, (values.shape[0], 128))

    def place_rows(group, segments):
        def one(b, carry):
            index = group * 16 + b
            row = index // segments
            j = iota((TILE, 128), 0)
            lane = iota((TILE, 128), 1).astype(jnp.float32)
            kept = jnp.full((TILE, 128), -1.0, jnp.float32)
            for k in range(CAP):
                if segments == 1:
                    at = columns[k, pl.ds(row, 1), :]
                else:
                    odd = jnp.full((1, 128), lax.rem(index, 2), jnp.int32)
                    at = jnp.where(odd == 0, columns[k, pl.ds(row, 1), :], columns[CAP + k, pl.ds(row, 1), :])
                kept = jnp.where(j == k, jnp.broadcast_to(at, (TILE, 128)), kept)
            for t in range(rows // 128):
                scratch[pl.ds(pl.multiple_of(b * TILE, TILE), TILE), t * 128 : (t + 1) * 128] = jnp.where(
                    kept == lane + float(t * 128), 1.0, 0.0
                )
            return carry

        lax.fori_loop(0, 16, one, 0)

    def turn(picker, group):
        for t in range(rows // 128):
            picker[t * 128 : (t + 1) * 128, pl.ds(pl.multiple_of(group * 128, 128), 128)] = jnp.transpose(
                scratch[:, t * 128 : (t + 1) * 128]
            ).astype(jnp.bfloat16)

    def over_groups(step):
        def one(group, carry):
            step(group)
            return carry

        return [lambda first=first: lax.fori_loop(first, first + 2, one, 0) for first in range(0, 8, 2)]

    def p2_group(group):
        place_rows(group, 2)
        turn(p2, group)

    def p3_group(group):
        place_rows(group, 1)
        p3[pl.ds(pl.multiple_of(group * 128, 128), 128), :] = scratch[...].astype(jnp.bfloat16)

    def codes(values, segment):
        n = values.shape[1]
        owner = iota((OWNERS, n), 0)
        spread = jnp.broadcast_to(values, (OWNERS, n))
        marked = (spread >= owner * rows) & (spread < owner * rows + rows)
        rank = prefix(marked, segment)
        code = (owner * TILE).astype(jnp.float32) + rank - 1.0
        return jnp.sum(jnp.where(marked, code, 0.0), axis=0, keepdims=True)

    def p1_all():
        both = codes(map_table[pl.ds(child * (CHIPS // 2) + chip // 2, 1), :], height)
        odd = jnp.full((1, height), lax.rem(chip, 2), jnp.int32)
        code = jnp.where(odd == 0, both[:, 0:height], both[:, height : 2 * height])

        def some(i, carry):
            slot = iota((128, height), 0)
            j = slot & (TILE - 1)
            wanted = jnp.where(j < CAP, slot, -(10**6)) + i * 128
            p1[pl.ds(pl.multiple_of(i * 128, 128), 128), :] = jnp.where(
                wanted.astype(jnp.float32) == jnp.broadcast_to(code, (128, height)), 1.0, 0.0
            ).astype(jnp.bfloat16)
            return carry

        lax.fori_loop(0, OWNERS * TILE // 128, some, 0)

    def p4_codes():
        mine = [leaf_rows[pl.ds(me * CAP + c, 1), :] for c in range(CAP)]
        code = codes(jnp.concatenate(mine, axis=1), rows)
        columns[0, 0:CAP, :] = jnp.concatenate([code[:, c * 128 : (c + 1) * 128] for c in range(CAP)], axis=0)

    def p4_group(group):
        for t in range(CAP):
            code = jnp.broadcast_to(columns[0, t : t + 1, :], (128, 128))
            slot = (iota((128, 128), 0) + group * 128).astype(jnp.float32)
            scratch[:, t * 128 : (t + 1) * 128] = jnp.where(slot == code, 1.0, 0.0)
        turn(p4, group)

    def leaf_places():
        inputs[1].wait()
        find_places(
            jnp.concatenate([leaf_rows[pl.ds(c, OWNERS, stride=CAP), :] for c in range(CAP)], axis=1), rows
        )

    def own_rows():
        inputs[2].wait()
        inputs[3].wait()
        leaf = block.shape[1]
        for b in range(rows // leaf):
            value = jnp.dot(
                block[b * leaf : (b + 1) * leaf, :],
                parent_omega[b * leaf : (b + 1) * leaf, :],
                preferred_element_type=jnp.float32,
            )
            stacked[b * leaf : (b + 1) * leaf, :] = value[:, :128]
            stacked[rows + b * leaf : rows + (b + 1) * leaf, :] = value[:, 128:]

    jobs = [start_loads, clear, map_in, lambda: find_places(map_table[...], height)]
    jobs += over_groups(p2_group)
    jobs += [p1_all, leaf_places]
    jobs += over_groups(p3_group)
    jobs += [p4_codes]
    jobs += over_groups(p4_group)
    jobs += [own_rows]

    own.wait()
    pl.semaphore_wait(barrier, 7)
    slots, arrived = make_schedule(WINDOW)
    ready = [ready_slot(batch, arrived) for batch in BATCHES]
    done = 0
    for t in range(len(slots) + WINDOW):
        if t >= WINDOW:
            wait_slot(t - WINDOW)
        if t < len(slots):
            for link, offset, part, half in slots[t]:
                data = piece(offset, part, half)
                pltpu.make_async_remote_copy(
                    data, data, sent_sem, slot_sem.at[t], device_id=(child, neighbour[link]), device_id_type=MESH
                ).start()
        if t >= WINDOW - 1 and jobs:
            jobs.pop(0)()
        if t == len(slots) + WINDOW - 1:
            pl.semaphore_signal(mate_sem, inc=1, device_id=(1 - child, chip), device_id_type=MESH)
        while done < len(BATCHES) and ready[done] <= t - WINDOW:
            multiply(done)
            done += 1

    def fill(send, picker, values):
        both = two_parts(values)

        def some(i, carry):
            tile = picked(picker[pl.ds(pl.multiple_of(i * 512, 512), 512), :], both)
            send[pl.ds(pl.multiple_of(i * (512 // TILE), 512 // TILE), 512 // TILE)] = tile.reshape(512 // TILE, TILE, 128)
            return carry

        lax.fori_loop(0, OWNERS * TILE // 512, some, 0)

    used = pl.ds(0, CAP)
    order = []
    for dx in range(SIDE):
        for dy in range(SIDE):
            for dz in range(SIDE):
                for other in range(2):
                    far = sum(min(v, SIDE - v) for v in (dx, dy, dz))
                    if far or other:
                        order.append((-far, dx, dy, dz, other))
    order.sort()

    def exchange(send, recv, sent_sem, came_sem):
        for _, dx, dy, dz, other in order:
            to = source((dx, dy, dz))
            kid = 1 - child if other else child
            pltpu.make_async_remote_copy(
                send.at[kid * CHIPS + to, used],
                recv.at[me, used],
                sent_sem,
                came_sem,
                device_id=(kid, to),
                device_id_type=MESH,
            ).start()
        recv[me] = send[me]
        most = pl.ds(0, OWNERS - 1)
        return pltpu.make_async_remote_copy(
            send.at[most, used],
            recv.at[most, used],
            sent_sem,
            came_sem,
            device_id=(child, neighbour[0, 1]),
            device_id_type=MESH,
        )

    def here(side):
        return slice(side * rows, (side + 1) * rows)

    first, second = [], []
    for side in range(2):
        fill(send1.at[side], p1, total[:, side * 128 : (side + 1) * 128])
        if side == 0:
            pl.semaphore_wait(mate_sem, 1)
        first.append(exchange(send1.at[side], recv1.at[side], sent1.at[side], came1.at[side]))
    for side in range(2):
        first[side].wait_recv()
        parts[...] = two_parts(recv1[side].reshape(OWNERS * TILE, 128))
        fill(send2.at[side], p3, stacked[here(side), :] + picked(p2[...], parts[...]))
        second.append(exchange(send2.at[side], recv2.at[side], sent2.at[side], came2.at[side]))
    for side in range(2):
        second[side].wait_recv()
        parts[...] = two_parts(recv2[side].reshape(OWNERS * TILE, 128))
        out_rows[here(side), :] = picked(p4[...], parts[...])
    for copy in first + second:
        copy.wait_send()
    sent = gathered.at[pl.ds(0, 6 * PIECE * len(slots))]
    pltpu.make_async_remote_copy(
        sent, sent, sent_sem, slot_sem.at[0], device_id=(child, neighbour[0, 1]), device_id_type=MESH
    ).wait_send()


def body(front_update, child_omega, parent_block, parent_omega, child_map, leaf_order):
    local_rows = front_update.shape[1]
    sample_cols = child_omega.shape[2]
    parent_dev, leaf_size = parent_block.shape
    slots, _ = make_schedule(WINDOW)
    vmem = pl.BlockSpec(memory_space=pltpu.VMEM)
    anywhere = pl.BlockSpec(memory_space=pl.ANY)
    tiles = pltpu.VMEM((2, OWNERS, TILE, 128), jnp.float32)
    slot_rows = OWNERS * TILE
    dma = pltpu.SemaphoreType.DMA
    result = pl.pallas_call(
        kernel,
        out_shape=jax.ShapeDtypeStruct((2 * parent_dev, 128), jnp.float32),
        in_specs=[anywhere] * 6,
        out_specs=vmem,
        scratch_shapes=[
            pltpu.VMEM((CHIPS * SHARD, sample_cols), jnp.bfloat16),
            pltpu.VMEM((CHIPS // 2, local_rows, PAIR), jnp.bfloat16),
            pltpu.VMEM((local_rows, sample_cols), jnp.float32),
            pltpu.VMEM((2 * parent_dev, 128), jnp.float32),
            pltpu.VMEM((slot_rows, 256), jnp.bfloat16),
            tiles,
            tiles,
            tiles,
            tiles,
            pltpu.VMEM((slot_rows, local_rows), jnp.bfloat16),
            pltpu.VMEM((parent_dev, slot_rows), jnp.bfloat16),
            pltpu.VMEM((slot_rows, parent_dev), jnp.bfloat16),
            pltpu.VMEM((parent_dev, slot_rows), jnp.bfloat16),
            pltpu.VMEM((parent_dev, leaf_size), jnp.bfloat16),
            pltpu.VMEM((parent_dev, sample_cols), jnp.bfloat16),
            pltpu.VMEM(child_map.shape, jnp.int32),
            pltpu.VMEM((parent_dev, 128), jnp.int32),
            pltpu.VMEM((OWNERS // 2, 2 * local_rows), jnp.int32),
            pltpu.VMEM((2 * CAP, OWNERS, 128), jnp.float32),
            pltpu.VMEM((128, parent_dev), jnp.float32),
            dma,
            dma((CHIPS // 2,)),
            dma((4,)),
            dma,
            dma((len(slots),)),
            pltpu.SemaphoreType.REGULAR,
            dma((2,)),
            dma((2,)),
            dma((2,)),
            dma((2,)),
        ],
        compiler_params=pltpu.CompilerParams(
            collective_id=0, has_side_effects=True, vmem_limit_bytes=67043328
        ),
    )(front_update, child_omega, parent_block, parent_omega, child_map, leaf_order.reshape(parent_dev, 128))
    return jnp.concatenate([result[:parent_dev], result[parent_dev:]], axis=1)


def solution(mesh):
    placed = (
        P("child", "rows", None),
        P("child", "rows", None),
        P(("child", "rows"), None),
        P(("child", "rows"), None),
        P(),
        P(),
    )
    return jax.shard_map(
        body, mesh=mesh, in_specs=placed, out_specs=P(("child", "rows"), None), check_vma=False
    )
```

```python
import functools

import jax
import jax.numpy as jnp
from jax import lax
from jax.experimental import pallas as pl
from jax.experimental.pallas import tpu as pltpu
from jax.sharding import PartitionSpec as P

MESH = pl.DeviceIdType.MESH
SIDE = 4
CHIPS = SIDE**3
OWNERS = 2 * CHIPS
SHARD = 960
THIRD = 256
REST = SHARD - 3 * THIRD
PAIR = 2 * SHARD
CAP = 3
TILE = 8
WINDOW = 4
UNIT = 64
STEP = 2


def drop_bit(r, d):
    return ((r >> (d + 1)) << d) | (r & ((1 << d) - 1))


def chunk_sets():
    found = []
    for d in range(3):
        e, f = (d + 1) % 3, (d + 2) % 3
        for h, links in enumerate(((e, 3 + d, f, 3 + e, 3 + f), (f, 3 + d, e, 3 + f, 3 + e))):
            found.append((("T", d, h), links, (0.0, 1.0, 2.0, 3.0, 4.0), 2))
    for i in range(3):
        b, c = (i + 1) % 3, (i + 2) % 3
        found.append((("R", i, 0), (i, b, 3 + i, 3 + b, c, 3 + c), (0.5, 1.5, 2.5, 3.5, 3.7, 9.0), 1))
    return found


def all_sends():
    sends = [[] for _ in range(6)]
    for name, links, ranks, size in chunk_sets():
        held = [0]
        for link, rank in zip(links, ranks):
            for r in held:
                order = (bin(r >> 3).count("1"), r >> 3, r) if rank == 9.0 else (0, 0, 0)
                sends[link].append((rank, order, name, r, size))
            held = held + [r ^ (1 << link) for r in held]
    for d in range(3):
        for r in range(CHIPS):
            if (r >> d) & 1:
                sends[d].append((5.0, (0, 0, drop_bit(r, d)), ("F", d, 0), r, 3))
        sends[d].append((6.0, (0, 0, 0), ("S", d, 0), 0, 6))
    return [sorted(found) for found in sends]


def loaded_step(r):
    return 3 + r // 16


T_BATCHES = tuple((d, 8 * g, 8) for g in range(4) for d in range(3))
R_BATCHES = tuple((4 * m, 4) for m in (0, 1, 2, 4, 3, 5, 6)) + tuple((28 + i, 1) for i in range(4))


def insert_bit(idx, d):
    return ((idx >> d) << (d + 1)) | (idx & ((1 << d) - 1))


def t_ready(batch, arrived):
    d, first, count = batch
    latest = 0
    for idx in range(first, first + count):
        r = insert_bit(idx, d)
        for key in ((("T", d, 0), r), (("T", d, 1), r), (("F", d, 0), r)):
            latest = max(latest, arrived.get(key, 10**6))
    return latest


def r_ready(batch, arrived):
    first, count = batch
    return max(arrived.get((("R", i, 0), r), 10**6) for i in range(3) for r in range(2 * first, 2 * (first + count)))


def make_schedule(window):
    waiting = all_sends()
    arrived = {(name, 0): -window for name, _, _, _ in chunk_sets()}
    free = [0] * 6
    steps = []
    while any(waiting):
        t = len(steps)
        now, came = [], []
        for link in range(6):
            free[link] = max(free[link], STEP * t)
            while free[link] < STEP * (t + 1):
                chosen = None
                for item in waiting[link]:
                    _, _, name, r, size = item
                    if name[0] == "F":
                        fit = loaded_step(r) <= t
                    elif name[0] == "S":
                        last = max(t_ready(b, arrived) for b in T_BATCHES if b[0] == name[1])
                        fit = last + window + 1 <= t
                    else:
                        fit = arrived.get((name, r), 10**6) + window <= t
                    if fit:
                        chosen = item
                        break
                if chosen is None:
                    break
                waiting[link].remove(chosen)
                _, _, name, r, size = chosen
                free[link] += size
                now.append((link, name, r, size))
                came.append((name, r ^ (1 << link)))
        for key in came:
            assert key not in arrived
            arrived[key] = t
        steps.append(now)
        assert t < 200
    return steps, arrived


def two_parts(values):
    high = values.astype(jnp.bfloat16)
    low = (values - high.astype(jnp.float32)).astype(jnp.bfloat16)
    return jnp.concatenate([high, low], axis=-1)


def picked(picker, parts):
    both = jnp.dot(picker, parts, preferred_element_type=jnp.float32)
    return both[:, :128] + both[:, 128:]


def kernel(
    front, omega, block_in, parent_in, child_map, leaf_order, out_rows,
    thirds, rests, slab_t, slab_r, lent, total, partial, came, stacked, parts, send1, recv1, send2, recv2, p1, p2, p3, p4,
    block, parent_omega, map_rows, leaf_rows, map_table, columns, scratch,
    own_sem, t_sem, r_sem, in_sem, sent_sem, slot_sem, mate_sem, sent1, came1, sent2, came2,
):
    child = lax.axis_index("child")
    chip = lax.axis_index("rows")
    me = child * CHIPS + chip
    place = (lax.rem(chip, SIDE), lax.rem(chip // SIDE, SIDE), chip // (SIDE * SIDE))
    back = []
    for d in range(3):
        v = place[d]
        flipped = v + 1 - 2 * lax.rem(v, 2)
        back.append([v, flipped, 3 - v, 3 - flipped])
    odd = lax.rem(place[0], 2)
    height = total.shape[0]
    rows = block.shape[0]

    def chip_at(xyz):
        return xyz[2] * (SIDE * SIDE) + xyz[1] * SIDE + xyz[0]

    def source(r):
        return chip_at([back[d][((r >> d) & 1) + 2 * ((r >> (3 + d)) & 1)] for d in range(3)])

    neighbour = [source(1 << link) for link in range(6)]

    own = [
        pltpu.make_async_copy(
            omega.at[0, pl.ds(pl.multiple_of(REST * odd + d * THIRD, UNIT), THIRD)],
            thirds.at[pl.ds(d * (CHIPS // 2) * THIRD, THIRD)],
            own_sem.at[d],
        )
        for d in range(3)
    ]
    own.append(
        pltpu.make_async_copy(
            omega.at[0, pl.ds(pl.multiple_of(3 * THIRD * (1 - odd), UNIT), REST)],
            rests.at[pl.ds(pl.multiple_of(REST * odd, UNIT), REST)],
            own_sem.at[3],
        )
    )
    for copy in own:
        copy.start()
    barrier = pltpu.get_barrier_semaphore()
    for there in neighbour:
        pl.semaphore_signal(barrier, inc=1, device_id=(child, there), device_id_type=MESH)
    pl.semaphore_signal(barrier, inc=1, device_id=(1 - child, chip), device_id_type=MESH)

    def coordinates(r):
        found = []
        for d in range(3):
            v = place[d]
            v = v + lax.rem(r // (1 << d), 2) * (1 - 2 * lax.rem(v, 2))
            found.append(v + lax.rem(r // (1 << (3 + d)), 2) * (3 - 2 * v))
        return found

    def t_copy(r):
        xyz = coordinates(r)
        at = (chip_at(xyz) // 2) * PAIR + lax.rem(xyz[0], 2) * (3 * THIRD + 2 * REST)
        return pltpu.make_async_copy(
            front.at[0, :, pl.ds(pl.multiple_of(at, 128), 3 * THIRD)], slab_t.at[r], t_sem.at[r]
        )

    def r_copy(idx):
        at = (chip_at(coordinates(2 * idx)) // 2) * PAIR + 3 * THIRD
        return pltpu.make_async_copy(
            front.at[0, :, pl.ds(pl.multiple_of(at, 128), 2 * REST)], slab_r.at[idx], r_sem.at[idx]
        )

    def each(first, count, step):
        def one(i, carry):
            step(i)
            return carry

        lax.fori_loop(first, first + count, one, 0)

    inputs = [
        pltpu.make_async_copy(source_ref, kept, in_sem.at[i])
        for i, (source_ref, kept) in enumerate(
            ((child_map, map_rows), (leaf_order, leaf_rows), (block_in, block), (parent_in, parent_omega))
        )
    ]

    each(0, CHIPS, lambda r: t_copy(r).start())

    def start_loads():
        for copy in inputs:
            copy.start()
        each(0, CHIPS // 2, lambda idx: r_copy(idx).start())
        total[...] = jnp.zeros_like(total)
        partial[...] = jnp.zeros_like(partial)

    def piece(name, r, base):
        kind, d, h = name
        if kind == "T":
            return thirds.at[pl.ds((d * (CHIPS // 2) + drop_bit(r, d)) * THIRD + h * (THIRD // 2), THIRD // 2)]
        parity = odd if (base & 1) == ((base >> 3) & 1) else 1 - odd
        at = (r >> 1) * (2 * REST) + d * UNIT + REST * parity
        return rests.at[pl.ds(pl.multiple_of(at, UNIT), UNIT)]

    def send(t, link, name, r):
        kind, d, _ = name
        if kind == "F":
            data = slab_t.at[r, :, pl.ds(d * THIRD, THIRD)]
            into = lent.at[d * (CHIPS // 2) + drop_bit(r, d)]
        elif kind == "S":
            data, into = partial.at[d], came.at[d]
        else:
            data, into = piece(name, r, r), piece(name, r ^ (1 << link), r)
        pltpu.make_async_remote_copy(
            data, into, sent_sem.at[link], slot_sem.at[t], device_id=(child, neighbour[link]), device_id_type=MESH
        ).start()

    def wait_units(units, sent, arrival):
        some = thirds.at[pl.ds(0, units * UNIT)]
        return pltpu.make_async_remote_copy(
            some, some, sent, arrival, device_id=(child, neighbour[0]), device_id_type=MESH
        )

    def multiply_t(batch):
        d, first, count = batch

        def two(i):
            low = 1 << d
            r = [(idx // low) * (2 * low) + lax.rem(idx, low) for idx in (2 * i, 2 * i + 1)]
            at = (d * (CHIPS // 2) + 2 * i) * THIRD
            right = thirds[pl.ds(pl.multiple_of(at, THIRD), 2 * THIRD), :]
            left = jnp.concatenate([slab_t[r[0], :, d * THIRD : (d + 1) * THIRD], slab_t[r[1], :, d * THIRD : (d + 1) * THIRD]], axis=1)
            total[...] += jnp.dot(left, right, preferred_element_type=jnp.float32)
            left = jnp.concatenate([lent[d * (CHIPS // 2) + 2 * i], lent[d * (CHIPS // 2) + 2 * i + 1]], axis=1)
            partial[d] += jnp.dot(left, right, preferred_element_type=jnp.float32)

        each(first // 2, count // 2, two)

    def multiply_r(batch):
        first, count = batch

        def one(idx):
            r_copy(idx).wait()
            right = rests[pl.ds(pl.multiple_of(idx * (2 * REST), 2 * REST), 2 * REST), :]
            total[...] += jnp.dot(slab_r[idx], right, preferred_element_type=jnp.float32)

        each(first, count, one)

    def clear():
        recv1[...] = jnp.zeros_like(recv1)
        recv2[...] = jnp.zeros_like(recv2)

    def map_in():
        inputs[0].wait()
        for u in range(CHIPS // 2):
            for c in range(2):
                map_table[c * (CHIPS // 2) + u : c * (CHIPS // 2) + u + 1, :] = map_rows[
                    c : c + 1, u * 2 * height : (u + 1) * 2 * height
                ]

    def iota(shape, dim):
        return lax.broadcasted_iota(jnp.int32, shape, dim)

    def upto(n, segment):
        i, j = iota((n, n), 0), iota((n, n), 1)
        same = i <= j
        if segment < n:
            same = same & ((i >= segment) == (j >= segment))
        return jnp.where(same, 1.0, 0.0).astype(jnp.bfloat16)

    def prefix(marked, segment):
        ones = jnp.where(marked, 1.0, 0.0).astype(jnp.bfloat16)
        return jnp.dot(ones, upto(marked.shape[1], segment), preferred_element_type=jnp.float32)

    def find_places(values, segment):
        low = me * rows
        marked = (values >= low) & (values < low + rows)
        rank = prefix(marked, segment)
        local = (values - low + 1).astype(jnp.float32)
        n = values.shape[1]
        lane = iota(values.shape, 1)
        for e in range(n // segment):
            inside = marked & (lane >= e * segment) & (lane < (e + 1) * segment)
            for k in range(CAP):
                found = jnp.sum(jnp.where(inside & (rank == k + 1.0), local, 0.0), axis=1, keepdims=True) - 1.0
                columns[e * CAP + k, 0 : values.shape[0], :] = jnp.broadcast_to(found, (values.shape[0], 128))

    def place_rows(group, segments):
        def one(b, carry):
            index = group * 16 + b
            row = index // segments
            j = iota((TILE, 128), 0)
            lane = iota((TILE, 128), 1).astype(jnp.float32)
            kept = jnp.full((TILE, 128), -1.0, jnp.float32)
            for k in range(CAP):
                if segments == 1:
                    at = columns[k, pl.ds(row, 1), :]
                else:
                    odd = jnp.full((1, 128), lax.rem(index, 2), jnp.int32)
                    at = jnp.where(odd == 0, columns[k, pl.ds(row, 1), :], columns[CAP + k, pl.ds(row, 1), :])
                kept = jnp.where(j == k, jnp.broadcast_to(at, (TILE, 128)), kept)
            for t in range(rows // 128):
                scratch[pl.ds(pl.multiple_of(b * TILE, TILE), TILE), t * 128 : (t + 1) * 128] = jnp.where(
                    kept == lane + float(t * 128), 1.0, 0.0
                )
            return carry

        lax.fori_loop(0, 16, one, 0)

    def turn(picker, group):
        for t in range(rows // 128):
            picker[t * 128 : (t + 1) * 128, pl.ds(pl.multiple_of(group * 128, 128), 128)] = jnp.transpose(
                scratch[:, t * 128 : (t + 1) * 128]
            ).astype(jnp.bfloat16)

    def over_groups(step):
        def one(group, carry):
            step(group)
            return carry

        return [lambda first=first: lax.fori_loop(first, first + 2, one, 0) for first in range(0, 8, 2)]

    def p2_group(group):
        place_rows(group, 2)
        turn(p2, group)

    def p3_group(group):
        place_rows(group, 1)
        p3[pl.ds(pl.multiple_of(group * 128, 128), 128), :] = scratch[...].astype(jnp.bfloat16)

    def codes(values, segment):
        n = values.shape[1]
        owner = iota((OWNERS, n), 0)
        spread = jnp.broadcast_to(values, (OWNERS, n))
        marked = (spread >= owner * rows) & (spread < owner * rows + rows)
        rank = prefix(marked, segment)
        code = (owner * TILE).astype(jnp.float32) + rank - 1.0
        return jnp.sum(jnp.where(marked, code, 0.0), axis=0, keepdims=True)

    def p1_all():
        both = codes(map_table[pl.ds(child * (CHIPS // 2) + chip // 2, 1), :], height)
        odd = jnp.full((1, height), lax.rem(chip, 2), jnp.int32)
        code = jnp.where(odd == 0, both[:, 0:height], both[:, height : 2 * height])

        def some(i, carry):
            slot = iota((128, height), 0)
            j = slot & (TILE - 1)
            wanted = jnp.where(j < CAP, slot, -(10**6)) + i * 128
            p1[pl.ds(pl.multiple_of(i * 128, 128), 128), :] = jnp.where(
                wanted.astype(jnp.float32) == jnp.broadcast_to(code, (128, height)), 1.0, 0.0
            ).astype(jnp.bfloat16)
            return carry

        lax.fori_loop(0, OWNERS * TILE // 128, some, 0)

    def p4_codes():
        mine = [leaf_rows[pl.ds(me * CAP + c, 1), :] for c in range(CAP)]
        code = codes(jnp.concatenate(mine, axis=1), rows)
        columns[0, 0:CAP, :] = jnp.concatenate([code[:, c * 128 : (c + 1) * 128] for c in range(CAP)], axis=0)

    def p4_group(group):
        for t in range(CAP):
            code = jnp.broadcast_to(columns[0, t : t + 1, :], (128, 128))
            slot = (iota((128, 128), 0) + group * 128).astype(jnp.float32)
            scratch[:, t * 128 : (t + 1) * 128] = jnp.where(slot == code, 1.0, 0.0)
        turn(p4, group)

    def leaf_places():
        inputs[1].wait()
        find_places(
            jnp.concatenate([leaf_rows[pl.ds(c, OWNERS, stride=CAP), :] for c in range(CAP)], axis=1), rows
        )

    def own_rows():
        inputs[2].wait()
        inputs[3].wait()
        leaf = block.shape[1]
        for b in range(rows // leaf):
            value = jnp.dot(
                block[b * leaf : (b + 1) * leaf, :],
                parent_omega[b * leaf : (b + 1) * leaf, :],
                preferred_element_type=jnp.float32,
            )
            stacked[b * leaf : (b + 1) * leaf, :] = value[:, :128]
            stacked[rows + b * leaf : rows + (b + 1) * leaf, :] = value[:, 128:]

    jobs = [start_loads, clear, map_in, lambda: find_places(map_table[...], height)]
    jobs += over_groups(p2_group)
    jobs += [p1_all, leaf_places]
    jobs += over_groups(p3_group)
    jobs += [p4_codes]
    jobs += over_groups(p4_group)
    jobs += [own_rows]

    for copy in own:
        copy.wait()
    pl.semaphore_wait(barrier, 7)
    steps, arrived = make_schedule(WINDOW)
    pending = [(t_ready(batch, arrived), multiply_t, batch) for batch in T_BATCHES]
    pending += [(r_ready(batch, arrived), multiply_r, batch) for batch in R_BATCHES]
    pending.sort(key=lambda entry: entry[0])
    sent_units = [0] * 6
    for t in range(len(steps) + WINDOW):
        if t >= WINDOW:
            units = sum(size for _, _, _, size in steps[t - WINDOW])
            wait_units(units, sent_sem.at[0], slot_sem.at[t - WINDOW]).wait_recv()
        if loaded_step(0) <= t <= loaded_step(CHIPS - 1):
            each(16 * (t - loaded_step(0)), 16, lambda r: t_copy(r).wait())
        if t < len(steps):
            for link, name, r, size in steps[t]:
                send(t, link, name, r)
                sent_units[link] += size
        if t >= WINDOW - 2 and jobs:
            jobs.pop(0)()
        if t == len(steps) + WINDOW - 1:
            pl.semaphore_signal(mate_sem, inc=1, device_id=(1 - child, chip), device_id_type=MESH)
        while pending and pending[0][0] <= t - WINDOW:
            _, multiply, batch = pending.pop(0)
            multiply(batch)
    total[...] += came[0] + came[1] + came[2]

    def fill(send, picker, values):
        both = two_parts(values)

        def some(i, carry):
            tile = picked(picker[pl.ds(pl.multiple_of(i * 512, 512), 512), :], both)
            send[pl.ds(pl.multiple_of(i * (512 // TILE), 512 // TILE), 512 // TILE)] = tile.reshape(512 // TILE, TILE, 128)
            return carry

        lax.fori_loop(0, OWNERS * TILE // 512, some, 0)

    used = pl.ds(0, CAP)
    order = []
    for dx in range(SIDE):
        for dy in range(SIDE):
            for dz in range(SIDE):
                for other in range(2):
                    far = sum(min(v, SIDE - v) for v in (dx, dy, dz))
                    if far or other:
                        order.append((-far, dx, dy, dz, other))
    order.sort()

    def exchange(send, recv, sent_sem, came_sem):
        for _, dx, dy, dz, other in order:
            to = chip_at([lax.rem(place[i] + v, SIDE) for i, v in enumerate((dx, dy, dz))])
            kid = 1 - child if other else child
            pltpu.make_async_remote_copy(
                send.at[kid * CHIPS + to, used],
                recv.at[me, used],
                sent_sem,
                came_sem,
                device_id=(kid, to),
                device_id_type=MESH,
            ).start()
        recv[me] = send[me]
        most = pl.ds(0, OWNERS - 1)
        return pltpu.make_async_remote_copy(
            send.at[most, used],
            recv.at[most, used],
            sent_sem,
            came_sem,
            device_id=(child, neighbour[0]),
            device_id_type=MESH,
        )

    def here(side):
        return slice(side * rows, (side + 1) * rows)

    first, second = [], []
    for side in range(2):
        fill(send1.at[side], p1, total[:, side * 128 : (side + 1) * 128])
        if side == 0:
            pl.semaphore_wait(mate_sem, 1)
        first.append(exchange(send1.at[side], recv1.at[side], sent1.at[side], came1.at[side]))
    for side in range(2):
        first[side].wait_recv()
        parts[...] = two_parts(recv1[side].reshape(OWNERS * TILE, 128))
        fill(send2.at[side], p3, stacked[here(side), :] + picked(p2[...], parts[...]))
        second.append(exchange(send2.at[side], recv2.at[side], sent2.at[side], came2.at[side]))
    for side in range(2):
        second[side].wait_recv()
        parts[...] = two_parts(recv2[side].reshape(OWNERS * TILE, 128))
        out_rows[here(side), :] = picked(p4[...], parts[...])
    for copy in first + second:
        copy.wait_send()
    for link in range(6):
        wait_units(sent_units[link], sent_sem.at[link], slot_sem.at[0]).wait_send()


def body(front_update, child_omega, parent_block, parent_omega, child_map, leaf_order):
    local_rows = front_update.shape[1]
    sample_cols = child_omega.shape[2]
    parent_dev, leaf_size = parent_block.shape
    steps, _ = make_schedule(WINDOW)
    vmem = pl.BlockSpec(memory_space=pltpu.VMEM)
    anywhere = pl.BlockSpec(memory_space=pl.ANY)
    tiles = pltpu.VMEM((2, OWNERS, TILE, 128), jnp.float32)
    slot_rows = OWNERS * TILE
    dma = pltpu.SemaphoreType.DMA
    result = pl.pallas_call(
        kernel,
        out_shape=jax.ShapeDtypeStruct((2 * parent_dev, 128), jnp.float32),
        in_specs=[anywhere] * 6,
        out_specs=vmem,
        scratch_shapes=[
            pltpu.VMEM((3 * (CHIPS // 2) * THIRD, sample_cols), jnp.bfloat16),
            pltpu.VMEM((CHIPS * REST, sample_cols), jnp.bfloat16),
            pltpu.VMEM((CHIPS, local_rows, 3 * THIRD), jnp.bfloat16),
            pltpu.VMEM((CHIPS // 2, local_rows, 2 * REST), jnp.bfloat16),
            pltpu.VMEM((3 * (CHIPS // 2), local_rows, THIRD), jnp.bfloat16),
            pltpu.VMEM((local_rows, sample_cols), jnp.float32),
            pltpu.VMEM((3, local_rows, sample_cols), jnp.float32),
            pltpu.VMEM((3, local_rows, sample_cols), jnp.float32),
            pltpu.VMEM((2 * parent_dev, 128), jnp.float32),
            pltpu.VMEM((slot_rows, 256), jnp.bfloat16),
            tiles,
            tiles,
            tiles,
            tiles,
            pltpu.VMEM((slot_rows, local_rows), jnp.bfloat16),
            pltpu.VMEM((parent_dev, slot_rows), jnp.bfloat16),
            pltpu.VMEM((slot_rows, parent_dev), jnp.bfloat16),
            pltpu.VMEM((parent_dev, slot_rows), jnp.bfloat16),
            pltpu.VMEM((parent_dev, leaf_size), jnp.bfloat16),
            pltpu.VMEM((parent_dev, sample_cols), jnp.bfloat16),
            pltpu.VMEM(child_map.shape, jnp.int32),
            pltpu.VMEM((parent_dev, 128), jnp.int32),
            pltpu.VMEM((OWNERS // 2, 2 * local_rows), jnp.int32),
            pltpu.VMEM((2 * CAP, OWNERS, 128), jnp.float32),
            pltpu.VMEM((128, parent_dev), jnp.float32),
            dma((4,)),
            dma((CHIPS,)),
            dma((CHIPS // 2,)),
            dma((4,)),
            dma((6,)),
            dma((len(steps),)),
            pltpu.SemaphoreType.REGULAR,
            dma((2,)),
            dma((2,)),
            dma((2,)),
            dma((2,)),
        ],
        compiler_params=pltpu.CompilerParams(
            collective_id=0, has_side_effects=True, vmem_limit_bytes=67043328
        ),
    )(front_update, child_omega, parent_block, parent_omega, child_map, leaf_order.reshape(parent_dev, 128))
    return jnp.concatenate([result[:parent_dev], result[parent_dev:]], axis=1)


def solution(mesh):
    placed = (
        P("child", "rows", None),
        P("child", "rows", None),
        P(("child", "rows"), None),
        P(("child", "rows"), None),
        P(),
        P(),
    )
    return jax.shard_map(
        body, mesh=mesh, in_specs=placed, out_specs=P(("child", "rows"), None), check_vma=False
    )
```

```python
import functools

import jax
import jax.numpy as jnp
from jax import lax
from jax.experimental import pallas as pl
from jax.experimental.pallas import tpu as pltpu
from jax.sharding import PartitionSpec as P

MESH = pl.DeviceIdType.MESH
SIDE = 4
CHIPS = SIDE**3
OWNERS = 2 * CHIPS
SHARD = 960
THIRD = 256
REST = SHARD - 3 * THIRD
PAIR = 2 * SHARD
CAP = 3
TILE = 8
WINDOW = 7
UNIT = 64
STEP = 2


def drop_bit(r, d):
    return ((r >> (d + 1)) << d) | (r & ((1 << d) - 1))


def chunk_sets():
    found = []
    for d in range(3):
        e, f = (d + 1) % 3, (d + 2) % 3
        for h, links in enumerate(((e, 3 + d, f, 3 + e, 3 + f), (f, 3 + d, e, 3 + f, 3 + e))):
            found.append((("T", d, h), links, (0.0, 1.0, 2.0, 3.0, 4.0), 2))
    for i in range(3):
        b, c = (i + 1) % 3, (i + 2) % 3
        found.append((("R", i, 0), (i, 3 + i, b, 3 + b, c, 3 + c), (0.5, 1.5, 2.5, 3.5, 3.7, 9.0), 1))
    return found


def all_sends():
    sends = [[] for _ in range(6)]
    for name, links, ranks, size in chunk_sets():
        held = [0]
        for link, rank in zip(links, ranks):
            for r in held:
                order = (bin(r >> 3).count("1"), r >> 3, r) if rank == 9.0 else (0, 0, 0)
                sends[link].append((rank, order, name, r, size))
            held = held + [r ^ (1 << link) for r in held]
    for d in range(3):
        for r in range(CHIPS):
            if (r >> d) & 1:
                sends[d].append((5.0, (0, 0, drop_bit(r, d)), ("F", d, 0), r, 3))
    return [sorted(found) for found in sends]


def loaded_step(r):
    return 3 + r // 16


T_BATCHES = tuple((d, 8 * g, 8) for g in range(3) for d in range(3)) + tuple((d, first, count) for first, count in ((24, 4), (28, 2), (30, 2)) for d in range(3))
R_BATCHES = tuple((4 * m, 4) for m in (0, 1, 2, 4, 3, 5, 6)) + tuple((28 + i, 1) for i in range(4))


def insert_bit(idx, d):
    return ((idx >> d) << (d + 1)) | (idx & ((1 << d) - 1))


def t_ready(batch, arrived):
    d, first, count = batch
    latest = 0
    for idx in range(first, first + count):
        r = insert_bit(idx, d)
        for key in ((("T", d, 0), r), (("T", d, 1), r), (("F", d, 0), r)):
            latest = max(latest, arrived.get(key, 10**6))
    return latest


def r_ready(batch, arrived):
    first, count = batch
    return max(arrived.get((("R", i, 0), r), 10**6) for i in range(3) for r in range(2 * first, 2 * (first + count)))


def make_schedule(window):
    waiting = all_sends()
    arrived = {(name, 0): -window for name, _, _, _ in chunk_sets()}
    free = [0] * 6
    steps = []
    while any(waiting):
        t = len(steps)
        now, came = [], []
        for link in range(6):
            free[link] = max(free[link], STEP * t)
            while free[link] < STEP * (t + 1):
                chosen = None
                for item in waiting[link]:
                    _, _, name, r, size = item
                    if name[0] == "F":
                        fit = loaded_step(r) <= t
                    else:
                        fit = arrived.get((name, r), 10**6) + window <= t
                    if fit:
                        chosen = item
                        break
                if chosen is None:
                    break
                waiting[link].remove(chosen)
                _, _, name, r, size = chosen
                free[link] += size
                now.append((link, name, r, size))
                came.append((name, r ^ (1 << link)))
        for key in came:
            assert key not in arrived
            arrived[key] = t
        steps.append(now)
        assert t < 200
    return steps, arrived


def two_parts(values):
    high = values.astype(jnp.bfloat16)
    low = (values - high.astype(jnp.float32)).astype(jnp.bfloat16)
    return jnp.concatenate([high, low], axis=-1)


def picked(picker, parts):
    both = jnp.dot(picker, parts, preferred_element_type=jnp.float32)
    return both[:, :128] + both[:, 128:]


def kernel(
    front, omega, block_in, parent_in, child_map, leaf_order, out_rows,
    thirds, rests, slab_t, slab_r, lent, total, partial, came, stacked, parts, send1, recv1, send2, recv2, p1, p2, p3, p4,
    block, parent_omega, map_rows, leaf_rows, map_table, columns, scratch,
    own_sem, t_sem, r_sem, in_sem, sent_sem, back_sem, slot_sem, mate_sem, sent1, came1, sent2, came2,
):
    child = lax.axis_index("child")
    chip = lax.axis_index("rows")
    me = child * CHIPS + chip
    place = (lax.rem(chip, SIDE), lax.rem(chip // SIDE, SIDE), chip // (SIDE * SIDE))
    back = []
    for d in range(3):
        v = place[d]
        flipped = v + 1 - 2 * lax.rem(v, 2)
        back.append([v, flipped, 3 - v, 3 - flipped])
    odd = lax.rem(place[0], 2)
    height = total.shape[0]
    rows = block.shape[0]

    def chip_at(xyz):
        return xyz[2] * (SIDE * SIDE) + xyz[1] * SIDE + xyz[0]

    def source(r):
        return chip_at([back[d][((r >> d) & 1) + 2 * ((r >> (3 + d)) & 1)] for d in range(3)])

    neighbour = [source(1 << link) for link in range(6)]

    own = [
        pltpu.make_async_copy(
            omega.at[0, pl.ds(pl.multiple_of(REST * odd + d * THIRD, UNIT), THIRD)],
            thirds.at[pl.ds(d * (CHIPS // 2) * THIRD, THIRD)],
            own_sem.at[d],
        )
        for d in range(3)
    ]
    own.append(
        pltpu.make_async_copy(
            omega.at[0, pl.ds(pl.multiple_of(3 * THIRD * (1 - odd), UNIT), REST)],
            rests.at[pl.ds(pl.multiple_of(REST * odd, UNIT), REST)],
            own_sem.at[3],
        )
    )
    for copy in own:
        copy.start()
    barrier = pltpu.get_barrier_semaphore()
    for there in neighbour:
        pl.semaphore_signal(barrier, inc=1, device_id=(child, there), device_id_type=MESH)
    pl.semaphore_signal(barrier, inc=1, device_id=(1 - child, chip), device_id_type=MESH)

    def coordinates(r):
        found = []
        for d in range(3):
            v = place[d]
            v = v + lax.rem(r // (1 << d), 2) * (1 - 2 * lax.rem(v, 2))
            found.append(v + lax.rem(r // (1 << (3 + d)), 2) * (3 - 2 * v))
        return found

    def t_copy(r):
        xyz = coordinates(r)
        at = (chip_at(xyz) // 2) * PAIR + lax.rem(xyz[0], 2) * (3 * THIRD + 2 * REST)
        return pltpu.make_async_copy(
            front.at[0, :, pl.ds(pl.multiple_of(at, 128), 3 * THIRD)], slab_t.at[r], t_sem.at[r]
        )

    def r_copy(idx):
        at = (chip_at(coordinates(2 * idx)) // 2) * PAIR + 3 * THIRD
        return pltpu.make_async_copy(
            front.at[0, :, pl.ds(pl.multiple_of(at, 128), 2 * REST)], slab_r.at[idx], r_sem.at[idx]
        )

    def each(first, count, step):
        def one(i, carry):
            step(i)
            return carry

        lax.fori_loop(first, first + count, one, 0)

    inputs = [
        pltpu.make_async_copy(source_ref, kept, in_sem.at[i])
        for i, (source_ref, kept) in enumerate(
            ((child_map, map_rows), (leaf_order, leaf_rows), (block_in, block), (parent_in, parent_omega))
        )
    ]

    each(0, CHIPS, lambda r: t_copy(r).start())

    def start_loads():
        for copy in inputs:
            copy.start()
        each(0, CHIPS // 2, lambda idx: r_copy(idx).start())
        total[...] = jnp.zeros_like(total)
        partial[...] = jnp.zeros_like(partial)

    def piece(name, r, base):
        kind, d, h = name
        if kind == "T":
            return thirds.at[pl.ds((d * (CHIPS // 2) + drop_bit(r, d)) * THIRD + h * (THIRD // 2), THIRD // 2)]
        parity = odd if (base & 1) == ((base >> 3) & 1) else 1 - odd
        at = (r >> 1) * (2 * REST) + d * UNIT + REST * parity
        return rests.at[pl.ds(pl.multiple_of(at, UNIT), UNIT)]

    def send(t, link, name, r):
        kind, d, _ = name
        if kind == "F":
            data = slab_t.at[r, :, pl.ds(d * THIRD, THIRD)]
            into = lent.at[d * (CHIPS // 2) + drop_bit(r, d)]
        else:
            data, into = piece(name, r, r), piece(name, r ^ (1 << link), r)
        pltpu.make_async_remote_copy(
            data, into, sent_sem.at[link], slot_sem.at[t], device_id=(child, neighbour[link]), device_id_type=MESH
        ).start()

    def lend_back(d):
        return pltpu.make_async_remote_copy(
            partial.at[d],
            came.at[d],
            back_sem.at[0, d],
            back_sem.at[1, d],
            device_id=(child, neighbour[d]),
            device_id_type=MESH,
        )

    def wait_units(units, sent, arrival):
        some = thirds.at[pl.ds(0, units * UNIT)]
        return pltpu.make_async_remote_copy(
            some, some, sent, arrival, device_id=(child, neighbour[0]), device_id_type=MESH
        )

    def multiply_t(batch):
        d, first, count = batch

        def two(i):
            low = 1 << d
            r = [(idx // low) * (2 * low) + lax.rem(idx, low) for idx in (2 * i, 2 * i + 1)]
            at = (d * (CHIPS // 2) + 2 * i) * THIRD
            right = thirds[pl.ds(pl.multiple_of(at, THIRD), 2 * THIRD), :]
            left = jnp.concatenate([slab_t[r[0], :, d * THIRD : (d + 1) * THIRD], slab_t[r[1], :, d * THIRD : (d + 1) * THIRD]], axis=1)
            total[...] += jnp.dot(left, right, preferred_element_type=jnp.float32)
            left = jnp.concatenate([lent[d * (CHIPS // 2) + 2 * i], lent[d * (CHIPS // 2) + 2 * i + 1]], axis=1)
            partial[d] += jnp.dot(left, right, preferred_element_type=jnp.float32)

        each(first // 2, count // 2, two)

    def multiply_r(batch):
        first, count = batch

        def one(idx):
            r_copy(idx).wait()
            right = rests[pl.ds(pl.multiple_of(idx * (2 * REST), 2 * REST), 2 * REST), :]
            total[...] += jnp.dot(slab_r[idx], right, preferred_element_type=jnp.float32)

        each(first, count, one)

    def clear():
        recv1[...] = jnp.zeros_like(recv1)
        recv2[...] = jnp.zeros_like(recv2)

    def map_in():
        inputs[0].wait()
        for u in range(CHIPS // 2):
            for c in range(2):
                map_table[c * (CHIPS // 2) + u : c * (CHIPS // 2) + u + 1, :] = map_rows[
                    c : c + 1, u * 2 * height : (u + 1) * 2 * height
                ]

    def iota(shape, dim):
        return lax.broadcasted_iota(jnp.int32, shape, dim)

    def upto(n, segment):
        i, j = iota((n, n), 0), iota((n, n), 1)
        same = i <= j
        if segment < n:
            same = same & ((i >= segment) == (j >= segment))
        return jnp.where(same, 1.0, 0.0).astype(jnp.bfloat16)

    def prefix(marked, segment):
        ones = jnp.where(marked, 1.0, 0.0).astype(jnp.bfloat16)
        return jnp.dot(ones, upto(marked.shape[1], segment), preferred_element_type=jnp.float32)

    def find_places(values, segment):
        low = me * rows
        marked = (values >= low) & (values < low + rows)
        rank = prefix(marked, segment)
        local = (values - low + 1).astype(jnp.float32)
        n = values.shape[1]
        lane = iota(values.shape, 1)
        for e in range(n // segment):
            inside = marked & (lane >= e * segment) & (lane < (e + 1) * segment)
            for k in range(CAP):
                found = jnp.sum(jnp.where(inside & (rank == k + 1.0), local, 0.0), axis=1, keepdims=True) - 1.0
                columns[e * CAP + k, 0 : values.shape[0], :] = jnp.broadcast_to(found, (values.shape[0], 128))

    def place_rows(group, segments):
        def one(b, carry):
            index = group * 16 + b
            row = index // segments
            j = iota((TILE, 128), 0)
            lane = iota((TILE, 128), 1).astype(jnp.float32)
            kept = jnp.full((TILE, 128), -1.0, jnp.float32)
            for k in range(CAP):
                if segments == 1:
                    at = columns[k, pl.ds(row, 1), :]
                else:
                    odd = jnp.full((1, 128), lax.rem(index, 2), jnp.int32)
                    at = jnp.where(odd == 0, columns[k, pl.ds(row, 1), :], columns[CAP + k, pl.ds(row, 1), :])
                kept = jnp.where(j == k, jnp.broadcast_to(at, (TILE, 128)), kept)
            for t in range(rows // 128):
                scratch[pl.ds(pl.multiple_of(b * TILE, TILE), TILE), t * 128 : (t + 1) * 128] = jnp.where(
                    kept == lane + float(t * 128), 1.0, 0.0
                )
            return carry

        lax.fori_loop(0, 16, one, 0)

    def turn(picker, group):
        for t in range(rows // 128):
            picker[t * 128 : (t + 1) * 128, pl.ds(pl.multiple_of(group * 128, 128), 128)] = jnp.transpose(
                scratch[:, t * 128 : (t + 1) * 128]
            ).astype(jnp.bfloat16)

    def over_groups(step):
        def one(group, carry):
            step(group)
            return carry

        return [lambda first=first: lax.fori_loop(first, first + 2, one, 0) for first in range(0, 8, 2)]

    def p2_group(group):
        place_rows(group, 2)
        turn(p2, group)

    def p3_group(group):
        place_rows(group, 1)
        p3[pl.ds(pl.multiple_of(group * 128, 128), 128), :] = scratch[...].astype(jnp.bfloat16)

    def codes(values, segment):
        n = values.shape[1]
        owner = iota((OWNERS, n), 0)
        spread = jnp.broadcast_to(values, (OWNERS, n))
        marked = (spread >= owner * rows) & (spread < owner * rows + rows)
        rank = prefix(marked, segment)
        code = (owner * TILE).astype(jnp.float32) + rank - 1.0
        return jnp.sum(jnp.where(marked, code, 0.0), axis=0, keepdims=True)

    def p1_all():
        both = codes(map_table[pl.ds(child * (CHIPS // 2) + chip // 2, 1), :], height)
        odd = jnp.full((1, height), lax.rem(chip, 2), jnp.int32)
        code = jnp.where(odd == 0, both[:, 0:height], both[:, height : 2 * height])

        def some(i, carry):
            slot = iota((128, height), 0)
            j = slot & (TILE - 1)
            wanted = jnp.where(j < CAP, slot, -(10**6)) + i * 128
            p1[pl.ds(pl.multiple_of(i * 128, 128), 128), :] = jnp.where(
                wanted.astype(jnp.float32) == jnp.broadcast_to(code, (128, height)), 1.0, 0.0
            ).astype(jnp.bfloat16)
            return carry

        lax.fori_loop(0, OWNERS * TILE // 128, some, 0)

    def p4_codes():
        mine = [leaf_rows[pl.ds(me * CAP + c, 1), :] for c in range(CAP)]
        code = codes(jnp.concatenate(mine, axis=1), rows)
        columns[0, 0:CAP, :] = jnp.concatenate([code[:, c * 128 : (c + 1) * 128] for c in range(CAP)], axis=0)

    def p4_group(group):
        for t in range(CAP):
            code = jnp.broadcast_to(columns[0, t : t + 1, :], (128, 128))
            slot = (iota((128, 128), 0) + group * 128).astype(jnp.float32)
            scratch[:, t * 128 : (t + 1) * 128] = jnp.where(slot == code, 1.0, 0.0)
        turn(p4, group)

    def leaf_places():
        inputs[1].wait()
        find_places(
            jnp.concatenate([leaf_rows[pl.ds(c, OWNERS, stride=CAP), :] for c in range(CAP)], axis=1), rows
        )

    def own_rows():
        inputs[2].wait()
        inputs[3].wait()
        leaf = block.shape[1]
        for b in range(rows // leaf):
            value = jnp.dot(
                block[b * leaf : (b + 1) * leaf, :],
                parent_omega[b * leaf : (b + 1) * leaf, :],
                preferred_element_type=jnp.float32,
            )
            stacked[b * leaf : (b + 1) * leaf, :] = value[:, :128]
            stacked[rows + b * leaf : rows + (b + 1) * leaf, :] = value[:, 128:]

    jobs = [start_loads, clear, map_in, lambda: find_places(map_table[...], height)]
    jobs += over_groups(p2_group)
    jobs += [p1_all, leaf_places]
    jobs += over_groups(p3_group)
    jobs += [p4_codes]
    jobs += over_groups(p4_group)
    jobs += [own_rows]

    for copy in own:
        copy.wait()
    pl.semaphore_wait(barrier, 7)
    steps, arrived = make_schedule(WINDOW)
    pending = [(t_ready(batch, arrived), multiply_t, batch) for batch in T_BATCHES]
    pending += [(r_ready(batch, arrived), multiply_r, batch) for batch in R_BATCHES]
    pending.sort(key=lambda entry: entry[0])
    sent_units = [0] * 6
    for t in range(len(steps) + WINDOW):
        if t >= WINDOW:
            units = sum(size for _, _, _, size in steps[t - WINDOW])
            wait_units(units, sent_sem.at[0], slot_sem.at[t - WINDOW]).wait_recv()
        if loaded_step(0) <= t <= loaded_step(CHIPS - 1):
            each(16 * (t - loaded_step(0)), 16, lambda r: t_copy(r).wait())
        if t < len(steps):
            for link, name, r, size in steps[t]:
                send(t, link, name, r)
                sent_units[link] += size
        if t >= WINDOW - 2 and jobs:
            jobs.pop(0)()
        if t == len(steps) + WINDOW - 1:
            pl.semaphore_signal(mate_sem, inc=1, device_id=(1 - child, chip), device_id_type=MESH)
        while pending and pending[0][0] <= t - WINDOW:
            _, multiply, batch = pending.pop(0)
            multiply(batch)
            if multiply is multiply_t and batch[1] + batch[2] == CHIPS // 2:
                lend_back(batch[0]).start()
    for d in range(3):
        lend_back(d).wait_recv()
        total[...] += came[d]

    def fill(send, picker, values):
        both = two_parts(values)

        def some(i, carry):
            tile = picked(picker[pl.ds(pl.multiple_of(i * 512, 512), 512), :], both)
            send[pl.ds(pl.multiple_of(i * (512 // TILE), 512 // TILE), 512 // TILE)] = tile.reshape(512 // TILE, TILE, 128)
            return carry

        lax.fori_loop(0, OWNERS * TILE // 512, some, 0)

    used = pl.ds(0, CAP)
    order = []
    for dx in range(SIDE):
        for dy in range(SIDE):
            for dz in range(SIDE):
                for other in range(2):
                    far = sum(min(v, SIDE - v) for v in (dx, dy, dz))
                    if far or other:
                        order.append((-far, dx, dy, dz, other))
    order.sort()

    def exchange(send, recv, sent_sem, came_sem):
        for _, dx, dy, dz, other in order:
            to = chip_at([lax.rem(place[i] + v, SIDE) for i, v in enumerate((dx, dy, dz))])
            kid = 1 - child if other else child
            pltpu.make_async_remote_copy(
                send.at[kid * CHIPS + to, used],
                recv.at[me, used],
                sent_sem,
                came_sem,
                device_id=(kid, to),
                device_id_type=MESH,
            ).start()
        recv[me] = send[me]
        most = pl.ds(0, OWNERS - 1)
        return pltpu.make_async_remote_copy(
            send.at[most, used],
            recv.at[most, used],
            sent_sem,
            came_sem,
            device_id=(child, neighbour[0]),
            device_id_type=MESH,
        )

    def here(side):
        return slice(side * rows, (side + 1) * rows)

    first, second = [], []
    for side in range(2):
        fill(send1.at[side], p1, total[:, side * 128 : (side + 1) * 128])
        if side == 0:
            pl.semaphore_wait(mate_sem, 1)
        first.append(exchange(send1.at[side], recv1.at[side], sent1.at[side], came1.at[side]))
    for side in range(2):
        first[side].wait_recv()
        parts[...] = two_parts(recv1[side].reshape(OWNERS * TILE, 128))
        fill(send2.at[side], p3, stacked[here(side), :] + picked(p2[...], parts[...]))
        second.append(exchange(send2.at[side], recv2.at[side], sent2.at[side], came2.at[side]))
    for side in range(2):
        second[side].wait_recv()
        parts[...] = two_parts(recv2[side].reshape(OWNERS * TILE, 128))
        out_rows[here(side), :] = picked(p4[...], parts[...])
    for copy in first + second:
        copy.wait_send()
    for d in range(3):
        lend_back(d).wait_send()
    for link in range(6):
        wait_units(sent_units[link], sent_sem.at[link], slot_sem.at[0]).wait_send()


def body(front_update, child_omega, parent_block, parent_omega, child_map, leaf_order):
    local_rows = front_update.shape[1]
    sample_cols = child_omega.shape[2]
    parent_dev, leaf_size = parent_block.shape
    steps, _ = make_schedule(WINDOW)
    vmem = pl.BlockSpec(memory_space=pltpu.VMEM)
    anywhere = pl.BlockSpec(memory_space=pl.ANY)
    tiles = pltpu.VMEM((2, OWNERS, TILE, 128), jnp.float32)
    slot_rows = OWNERS * TILE
    dma = pltpu.SemaphoreType.DMA
    result = pl.pallas_call(
        kernel,
        out_shape=jax.ShapeDtypeStruct((2 * parent_dev, 128), jnp.float32),
        in_specs=[anywhere] * 6,
        out_specs=vmem,
        scratch_shapes=[
            pltpu.VMEM((3 * (CHIPS // 2) * THIRD, sample_cols), jnp.bfloat16),
            pltpu.VMEM((CHIPS * REST, sample_cols), jnp.bfloat16),
            pltpu.VMEM((CHIPS, local_rows, 3 * THIRD), jnp.bfloat16),
            pltpu.VMEM((CHIPS // 2, local_rows, 2 * REST), jnp.bfloat16),
            pltpu.VMEM((3 * (CHIPS // 2), local_rows, THIRD), jnp.bfloat16),
            pltpu.VMEM((local_rows, sample_cols), jnp.float32),
            pltpu.VMEM((3, local_rows, sample_cols), jnp.float32),
            pltpu.VMEM((3, local_rows, sample_cols), jnp.float32),
            pltpu.VMEM((2 * parent_dev, 128), jnp.float32),
            pltpu.VMEM((slot_rows, 256), jnp.bfloat16),
            tiles,
            tiles,
            tiles,
            tiles,
            pltpu.VMEM((slot_rows, local_rows), jnp.bfloat16),
            pltpu.VMEM((parent_dev, slot_rows), jnp.bfloat16),
            pltpu.VMEM((slot_rows, parent_dev), jnp.bfloat16),
            pltpu.VMEM((parent_dev, slot_rows), jnp.bfloat16),
            pltpu.VMEM((parent_dev, leaf_size), jnp.bfloat16),
            pltpu.VMEM((parent_dev, sample_cols), jnp.bfloat16),
            pltpu.VMEM(child_map.shape, jnp.int32),
            pltpu.VMEM((parent_dev, 128), jnp.int32),
            pltpu.VMEM((OWNERS // 2, 2 * local_rows), jnp.int32),
            pltpu.VMEM((2 * CAP, OWNERS, 128), jnp.float32),
            pltpu.VMEM((128, parent_dev), jnp.float32),
            dma((4,)),
            dma((CHIPS,)),
            dma((CHIPS // 2,)),
            dma((4,)),
            dma((6,)),
            dma((2, 3)),
            dma((len(steps),)),
            pltpu.SemaphoreType.REGULAR,
            dma((2,)),
            dma((2,)),
            dma((2,)),
            dma((2,)),
        ],
        compiler_params=pltpu.CompilerParams(
            collective_id=0, has_side_effects=True, vmem_limit_bytes=67043328
        ),
    )(front_update, child_omega, parent_block, parent_omega, child_map, leaf_order.reshape(parent_dev, 128))
    return jnp.concatenate([result[:parent_dev], result[parent_dev:]], axis=1)


def solution(mesh):
    placed = (
        P("child", "rows", None),
        P("child", "rows", None),
        P(("child", "rows"), None),
        P(("child", "rows"), None),
        P(),
        P(),
    )
    return jax.shard_map(
        body, mesh=mesh, in_specs=placed, out_specs=P(("child", "rows"), None), check_vma=False
    )
```

```python
import functools

import jax
import jax.numpy as jnp
from jax import lax
from jax.experimental import pallas as pl
from jax.experimental.pallas import tpu as pltpu
from jax.sharding import PartitionSpec as P

MESH = pl.DeviceIdType.MESH
SIDE = 4
CHIPS = SIDE**3
OWNERS = 2 * CHIPS
SHARD = 960
THIRD = 256
REST = SHARD - 3 * THIRD
PAIR = 2 * SHARD
CAP = 3
TILE = 8
WINDOW = 7
UNIT = 64
STEP = 2


def drop_bit(r, d):
    return ((r >> (d + 1)) << d) | (r & ((1 << d) - 1))


def chunk_sets():
    found = []
    for d in range(3):
        e, f = (d + 1) % 3, (d + 2) % 3
        for h, links in enumerate(((e, 3 + d, f, 3 + e, 3 + f), (f, 3 + d, e, 3 + f, 3 + e))):
            found.append((("T", d, h), links, (0.0, 1.0, 2.0, 3.0, 4.0), 2))
    for i in range(3):
        b, c = (i + 1) % 3, (i + 2) % 3
        found.append((("R", i, 0), (3 + i, i, b, 3 + b, c, 3 + c), (0.5, 1.5, 2.5, 3.5, 3.7, 9.0), 1))
    return found


def all_sends():
    sends = [[] for _ in range(6)]
    for name, links, ranks, size in chunk_sets():
        held = [0]
        for link, rank in zip(links, ranks):
            for r in held:
                order = (bin(r >> 3).count("1"), r >> 3, r) if rank == 9.0 else (0, 0, 0)
                sends[link].append((rank, order, name, r, size))
            held = held + [r ^ (1 << link) for r in held]
    for d in range(3):
        for r in range(CHIPS):
            if (r >> d) & 1:
                sends[d].append((5.0, (0, 0, drop_bit(r, d)), ("F", d, 0), r, 3))
    return [sorted(found) for found in sends]


def loaded_step(r):
    return 3 + r // 16


T_BATCHES = tuple((d, 8 * g, 8) for g in range(3) for d in range(3)) + tuple((d, first, count) for first, count in ((24, 4), (28, 2), (30, 2)) for d in range(3))
R_BATCHES = tuple((4 * m, 4) for m in (0, 1, 2, 4, 3, 5, 6)) + tuple((28 + i, 1) for i in range(4))


def insert_bit(idx, d):
    return ((idx >> d) << (d + 1)) | (idx & ((1 << d) - 1))


def t_ready(batch, arrived):
    d, first, count = batch
    latest = 0
    for idx in range(first, first + count):
        r = insert_bit(idx, d)
        for key in ((("T", d, 0), r), (("T", d, 1), r), (("F", d, 0), r)):
            latest = max(latest, arrived.get(key, 10**6))
    return latest


def r_ready(batch, arrived):
    first, count = batch
    return max(arrived.get((("R", i, 0), r), 10**6) for i in range(3) for r in range(2 * first, 2 * (first + count)))


def make_schedule(window):
    waiting = all_sends()
    arrived = {(name, 0): -window for name, _, _, _ in chunk_sets()}
    free = [0] * 6
    steps = []
    while any(waiting):
        t = len(steps)
        now, came = [], []
        for link in range(6):
            free[link] = max(free[link], STEP * t)
            while free[link] < STEP * (t + 1):
                chosen = None
                for item in waiting[link]:
                    _, _, name, r, size = item
                    if name[0] == "F":
                        fit = loaded_step(r) <= t
                    else:
                        fit = arrived.get((name, r), 10**6) + window <= t
                    if fit:
                        chosen = item
                        break
                if chosen is None:
                    break
                waiting[link].remove(chosen)
                _, _, name, r, size = chosen
                free[link] += size
                now.append((link, name, r, size))
                came.append((name, r ^ (1 << link)))
        for key in came:
            assert key not in arrived
            arrived[key] = t
        steps.append(now)
        assert t < 200
    return steps, arrived


def two_parts(values):
    high = values.astype(jnp.bfloat16)
    low = (values - high.astype(jnp.float32)).astype(jnp.bfloat16)
    return jnp.concatenate([high, low], axis=-1)


def picked(picker, parts):
    both = jnp.dot(picker, parts, preferred_element_type=jnp.float32)
    return both[:, :128] + both[:, 128:]


def kernel(
    front, omega, block_in, parent_in, child_map, leaf_order, out_rows,
    thirds, rests, slab_t, slab_r, lent, total, partial, came, stacked, parts, send1, recv1, send2, recv2, p1, p2, p3, p4,
    block, parent_omega, map_rows, leaf_rows, map_table, columns, scratch,
    own_sem, t_sem, r_sem, in_sem, sent_sem, back_sem, slot_sem, mate_sem, sent1, came1, sent2, came2,
):
    child = lax.axis_index("child")
    chip = lax.axis_index("rows")
    me = child * CHIPS + chip
    place = (lax.rem(chip, SIDE), lax.rem(chip // SIDE, SIDE), chip // (SIDE * SIDE))
    back = []
    for d in range(3):
        v = place[d]
        flipped = v + 1 - 2 * lax.rem(v, 2)
        back.append([v, flipped, 3 - v, 3 - flipped])
    odd = lax.rem(place[0], 2)
    height = total.shape[0]
    rows = block.shape[0]

    def chip_at(xyz):
        return xyz[2] * (SIDE * SIDE) + xyz[1] * SIDE + xyz[0]

    def source(r):
        return chip_at([back[d][((r >> d) & 1) + 2 * ((r >> (3 + d)) & 1)] for d in range(3)])

    neighbour = [source(1 << link) for link in range(6)]

    own = [
        pltpu.make_async_copy(
            omega.at[0, pl.ds(pl.multiple_of(REST * odd + d * THIRD, UNIT), THIRD)],
            thirds.at[pl.ds(d * (CHIPS // 2) * THIRD, THIRD)],
            own_sem.at[d],
        )
        for d in range(3)
    ]
    own.append(
        pltpu.make_async_copy(
            omega.at[0, pl.ds(pl.multiple_of(3 * THIRD * (1 - odd), UNIT), REST)],
            rests.at[pl.ds(pl.multiple_of(REST * odd, UNIT), REST)],
            own_sem.at[3],
        )
    )
    for copy in own:
        copy.start()
    barrier = pltpu.get_barrier_semaphore()
    for there in neighbour:
        pl.semaphore_signal(barrier, inc=1, device_id=(child, there), device_id_type=MESH)
    pl.semaphore_signal(barrier, inc=1, device_id=(1 - child, chip), device_id_type=MESH)

    def coordinates(r):
        found = []
        for d in range(3):
            v = place[d]
            v = v + lax.rem(r // (1 << d), 2) * (1 - 2 * lax.rem(v, 2))
            found.append(v + lax.rem(r // (1 << (3 + d)), 2) * (3 - 2 * v))
        return found

    def t_copy(r):
        xyz = coordinates(r)
        at = (chip_at(xyz) // 2) * PAIR + lax.rem(xyz[0], 2) * (3 * THIRD + 2 * REST)
        return pltpu.make_async_copy(
            front.at[0, :, pl.ds(pl.multiple_of(at, 128), 3 * THIRD)], slab_t.at[r], t_sem.at[r]
        )

    def r_copy(idx):
        at = (chip_at(coordinates(2 * idx)) // 2) * PAIR + 3 * THIRD
        return pltpu.make_async_copy(
            front.at[0, :, pl.ds(pl.multiple_of(at, 128), 2 * REST)], slab_r.at[idx], r_sem.at[idx]
        )

    def each(first, count, step):
        def one(i, carry):
            step(i)
            return carry

        lax.fori_loop(first, first + count, one, 0)

    inputs = [
        pltpu.make_async_copy(source_ref, kept, in_sem.at[i])
        for i, (source_ref, kept) in enumerate(
            ((child_map, map_rows), (leaf_order, leaf_rows), (block_in, block), (parent_in, parent_omega))
        )
    ]

    each(0, CHIPS, lambda r: t_copy(r).start())

    def start_loads():
        for copy in inputs:
            copy.start()
        each(0, CHIPS // 2, lambda idx: r_copy(idx).start())
        total[...] = jnp.zeros_like(total)
        partial[...] = jnp.zeros_like(partial)

    def piece(name, r, base):
        kind, d, h = name
        if kind == "T":
            return thirds.at[pl.ds((d * (CHIPS // 2) + drop_bit(r, d)) * THIRD + h * (THIRD // 2), THIRD // 2)]
        parity = odd if (base & 1) == ((base >> 3) & 1) else 1 - odd
        at = (r >> 1) * (2 * REST) + d * UNIT + REST * parity
        return rests.at[pl.ds(pl.multiple_of(at, UNIT), UNIT)]

    def send(t, link, name, r):
        kind, d, _ = name
        if kind == "F":
            data = slab_t.at[r, :, pl.ds(d * THIRD, THIRD)]
            into = lent.at[d * (CHIPS // 2) + drop_bit(r, d)]
        else:
            data, into = piece(name, r, r), piece(name, r ^ (1 << link), r)
        pltpu.make_async_remote_copy(
            data, into, sent_sem.at[link], slot_sem.at[t], device_id=(child, neighbour[link]), device_id_type=MESH
        ).start()

    def lend_back(d):
        return pltpu.make_async_remote_copy(
            partial.at[d],
            came.at[d],
            back_sem.at[0, d],
            back_sem.at[1, d],
            device_id=(child, neighbour[d]),
            device_id_type=MESH,
        )

    def wait_units(units, sent, arrival):
        some = thirds.at[pl.ds(0, units * UNIT)]
        return pltpu.make_async_remote_copy(
            some, some, sent, arrival, device_id=(child, neighbour[0]), device_id_type=MESH
        )

    def multiply_t(batch):
        d, first, count = batch

        def two(i):
            low = 1 << d
            r = [(idx // low) * (2 * low) + lax.rem(idx, low) for idx in (2 * i, 2 * i + 1)]
            at = (d * (CHIPS // 2) + 2 * i) * THIRD
            right = thirds[pl.ds(pl.multiple_of(at, THIRD), 2 * THIRD), :]
            left = jnp.concatenate([slab_t[r[0], :, d * THIRD : (d + 1) * THIRD], slab_t[r[1], :, d * THIRD : (d + 1) * THIRD]], axis=1)
            total[...] += jnp.dot(left, right, preferred_element_type=jnp.float32)
            left = jnp.concatenate([lent[d * (CHIPS // 2) + 2 * i], lent[d * (CHIPS // 2) + 2 * i + 1]], axis=1)
            partial[d] += jnp.dot(left, right, preferred_element_type=jnp.float32)

        each(first // 2, count // 2, two)

    def multiply_r(batch):
        first, count = batch

        def one(idx):
            r_copy(idx).wait()
            right = rests[pl.ds(pl.multiple_of(idx * (2 * REST), 2 * REST), 2 * REST), :]
            total[...] += jnp.dot(slab_r[idx], right, preferred_element_type=jnp.float32)

        each(first, count, one)

    def clear():
        recv1[...] = jnp.zeros_like(recv1)
        recv2[...] = jnp.zeros_like(recv2)

    def map_in():
        inputs[0].wait()
        for u in range(CHIPS // 2):
            for c in range(2):
                map_table[c * (CHIPS // 2) + u : c * (CHIPS // 2) + u + 1, :] = map_rows[
                    c : c + 1, u * 2 * height : (u + 1) * 2 * height
                ]

    def iota(shape, dim):
        return lax.broadcasted_iota(jnp.int32, shape, dim)

    def upto(n, segment):
        i, j = iota((n, n), 0), iota((n, n), 1)
        same = i <= j
        if segment < n:
            same = same & ((i >= segment) == (j >= segment))
        return jnp.where(same, 1.0, 0.0).astype(jnp.bfloat16)

    def prefix(marked, segment):
        ones = jnp.where(marked, 1.0, 0.0).astype(jnp.bfloat16)
        return jnp.dot(ones, upto(marked.shape[1], segment), preferred_element_type=jnp.float32)

    def find_places(values, segment):
        low = me * rows
        marked = (values >= low) & (values < low + rows)
        rank = prefix(marked, segment)
        local = (values - low + 1).astype(jnp.float32)
        n = values.shape[1]
        lane = iota(values.shape, 1)
        for e in range(n // segment):
            inside = marked & (lane >= e * segment) & (lane < (e + 1) * segment)
            for k in range(CAP):
                found = jnp.sum(jnp.where(inside & (rank == k + 1.0), local, 0.0), axis=1, keepdims=True) - 1.0
                columns[e * CAP + k, 0 : values.shape[0], :] = jnp.broadcast_to(found, (values.shape[0], 128))

    def place_rows(group, segments):
        def one(b, carry):
            index = group * 16 + b
            row = index // segments
            j = iota((TILE, 128), 0)
            lane = iota((TILE, 128), 1).astype(jnp.float32)
            kept = jnp.full((TILE, 128), -1.0, jnp.float32)
            for k in range(CAP):
                if segments == 1:
                    at = columns[k, pl.ds(row, 1), :]
                else:
                    odd = jnp.full((1, 128), lax.rem(index, 2), jnp.int32)
                    at = jnp.where(odd == 0, columns[k, pl.ds(row, 1), :], columns[CAP + k, pl.ds(row, 1), :])
                kept = jnp.where(j == k, jnp.broadcast_to(at, (TILE, 128)), kept)
            for t in range(rows // 128):
                scratch[pl.ds(pl.multiple_of(b * TILE, TILE), TILE), t * 128 : (t + 1) * 128] = jnp.where(
                    kept == lane + float(t * 128), 1.0, 0.0
                )
            return carry

        lax.fori_loop(0, 16, one, 0)

    def turn(picker, group):
        for t in range(rows // 128):
            picker[t * 128 : (t + 1) * 128, pl.ds(pl.multiple_of(group * 128, 128), 128)] = jnp.transpose(
                scratch[:, t * 128 : (t + 1) * 128]
            ).astype(jnp.bfloat16)

    def over_groups(step):
        def one(group, carry):
            step(group)
            return carry

        return [lambda first=first: lax.fori_loop(first, first + 2, one, 0) for first in range(0, 8, 2)]

    def p2_group(group):
        place_rows(group, 2)
        turn(p2, group)

    def p3_group(group):
        place_rows(group, 1)
        p3[pl.ds(pl.multiple_of(group * 128, 128), 128), :] = scratch[...].astype(jnp.bfloat16)

    def codes(values, segment):
        n = values.shape[1]
        owner = iota((OWNERS, n), 0)
        spread = jnp.broadcast_to(values, (OWNERS, n))
        marked = (spread >= owner * rows) & (spread < owner * rows + rows)
        rank = prefix(marked, segment)
        code = (owner * TILE).astype(jnp.float32) + rank - 1.0
        return jnp.sum(jnp.where(marked, code, 0.0), axis=0, keepdims=True)

    def p1_all():
        both = codes(map_table[pl.ds(child * (CHIPS // 2) + chip // 2, 1), :], height)
        odd = jnp.full((1, height), lax.rem(chip, 2), jnp.int32)
        code = jnp.where(odd == 0, both[:, 0:height], both[:, height : 2 * height])

        def some(i, carry):
            slot = iota((128, height), 0)
            j = slot & (TILE - 1)
            wanted = jnp.where(j < CAP, slot, -(10**6)) + i * 128
            p1[pl.ds(pl.multiple_of(i * 128, 128), 128), :] = jnp.where(
                wanted.astype(jnp.float32) == jnp.broadcast_to(code, (128, height)), 1.0, 0.0
            ).astype(jnp.bfloat16)
            return carry

        lax.fori_loop(0, OWNERS * TILE // 128, some, 0)

    def p4_codes():
        mine = [leaf_rows[pl.ds(me * CAP + c, 1), :] for c in range(CAP)]
        code = codes(jnp.concatenate(mine, axis=1), rows)
        columns[0, 0:CAP, :] = jnp.concatenate([code[:, c * 128 : (c + 1) * 128] for c in range(CAP)], axis=0)

    def p4_group(group):
        for t in range(CAP):
            code = jnp.broadcast_to(columns[0, t : t + 1, :], (128, 128))
            slot = (iota((128, 128), 0) + group * 128).astype(jnp.float32)
            scratch[:, t * 128 : (t + 1) * 128] = jnp.where(slot == code, 1.0, 0.0)
        turn(p4, group)

    def leaf_places():
        inputs[1].wait()
        find_places(
            jnp.concatenate([leaf_rows[pl.ds(c, OWNERS, stride=CAP), :] for c in range(CAP)], axis=1), rows
        )

    def own_rows():
        inputs[2].wait()
        inputs[3].wait()
        leaf = block.shape[1]
        for b in range(rows // leaf):
            value = jnp.dot(
                block[b * leaf : (b + 1) * leaf, :],
                parent_omega[b * leaf : (b + 1) * leaf, :],
                preferred_element_type=jnp.float32,
            )
            stacked[b * leaf : (b + 1) * leaf, :] = value[:, :128]
            stacked[rows + b * leaf : rows + (b + 1) * leaf, :] = value[:, 128:]

    jobs = [start_loads, clear, map_in, lambda: find_places(map_table[...], height)]
    jobs += over_groups(p2_group)
    jobs += [p1_all, leaf_places]
    jobs += over_groups(p3_group)
    jobs += [p4_codes]
    jobs += over_groups(p4_group)
    jobs += [own_rows]

    for copy in own:
        copy.wait()
    pl.semaphore_wait(barrier, 7)
    steps, arrived = make_schedule(WINDOW)
    pending = [(t_ready(batch, arrived), multiply_t, batch) for batch in T_BATCHES]
    pending += [(r_ready(batch, arrived), multiply_r, batch) for batch in R_BATCHES]
    pending.sort(key=lambda entry: entry[0])
    sent_units = [0] * 6
    for t in range(len(steps) + WINDOW):
        if t >= WINDOW:
            units = sum(size for _, _, _, size in steps[t - WINDOW])
            wait_units(units, sent_sem.at[0], slot_sem.at[t - WINDOW]).wait_recv()
        if loaded_step(0) <= t <= loaded_step(CHIPS - 1):
            each(16 * (t - loaded_step(0)), 16, lambda r: t_copy(r).wait())
        if t < len(steps):
            for link, name, r, size in steps[t]:
                send(t, link, name, r)
                sent_units[link] += size
        if t >= WINDOW - 2 and jobs:
            jobs.pop(0)()
        if t == len(steps) + WINDOW - 1:
            pl.semaphore_signal(mate_sem, inc=1, device_id=(1 - child, chip), device_id_type=MESH)
        while pending and pending[0][0] <= t - WINDOW:
            _, multiply, batch = pending.pop(0)
            multiply(batch)
            if multiply is multiply_t and batch[1] + batch[2] == CHIPS // 2:
                lend_back(batch[0]).start()
    for d in range(3):
        lend_back(d).wait_recv()
        total[...] += came[d]

    def fill(send, picker, values):
        both = two_parts(values)

        def some(i, carry):
            tile = picked(picker[pl.ds(pl.multiple_of(i * 512, 512), 512), :], both)
            send[pl.ds(pl.multiple_of(i * (512 // TILE), 512 // TILE), 512 // TILE)] = tile.reshape(512 // TILE, TILE, 128)
            return carry

        lax.fori_loop(0, OWNERS * TILE // 512, some, 0)

    used = pl.ds(0, CAP)
    order = []
    for dx in range(SIDE):
        for dy in range(SIDE):
            for dz in range(SIDE):
                for other in range(2):
                    far = sum(min(v, SIDE - v) for v in (dx, dy, dz))
                    if far or other:
                        order.append((-far, dx, dy, dz, other))
    order.sort()

    def exchange(send, recv, sent_sem, came_sem):
        for _, dx, dy, dz, other in order:
            to = chip_at([lax.rem(place[i] + v, SIDE) for i, v in enumerate((dx, dy, dz))])
            kid = 1 - child if other else child
            pltpu.make_async_remote_copy(
                send.at[kid * CHIPS + to, used],
                recv.at[me, used],
                sent_sem,
                came_sem,
                device_id=(kid, to),
                device_id_type=MESH,
            ).start()
        recv[me] = send[me]
        most = pl.ds(0, OWNERS - 1)
        return pltpu.make_async_remote_copy(
            send.at[most, used],
            recv.at[most, used],
            sent_sem,
            came_sem,
            device_id=(child, neighbour[0]),
            device_id_type=MESH,
        )

    def here(side):
        return slice(side * rows, (side + 1) * rows)

    first, second = [], []
    for side in range(2):
        fill(send1.at[side], p1, total[:, side * 128 : (side + 1) * 128])
        if side == 0:
            pl.semaphore_wait(mate_sem, 1)
        first.append(exchange(send1.at[side], recv1.at[side], sent1.at[side], came1.at[side]))
    for side in range(2):
        first[side].wait_recv()
        parts[...] = two_parts(recv1[side].reshape(OWNERS * TILE, 128))
        fill(send2.at[side], p3, stacked[here(side), :] + picked(p2[...], parts[...]))
        second.append(exchange(send2.at[side], recv2.at[side], sent2.at[side], came2.at[side]))
    for side in range(2):
        second[side].wait_recv()
        parts[...] = two_parts(recv2[side].reshape(OWNERS * TILE, 128))
        out_rows[here(side), :] = picked(p4[...], parts[...])
    for copy in first + second:
        copy.wait_send()
    for d in range(3):
        lend_back(d).wait_send()
    for link in range(6):
        wait_units(sent_units[link], sent_sem.at[link], slot_sem.at[0]).wait_send()


def body(front_update, child_omega, parent_block, parent_omega, child_map, leaf_order):
    local_rows = front_update.shape[1]
    sample_cols = child_omega.shape[2]
    parent_dev, leaf_size = parent_block.shape
    steps, _ = make_schedule(WINDOW)
    vmem = pl.BlockSpec(memory_space=pltpu.VMEM)
    anywhere = pl.BlockSpec(memory_space=pl.ANY)
    tiles = pltpu.VMEM((2, OWNERS, TILE, 128), jnp.float32)
    slot_rows = OWNERS * TILE
    dma = pltpu.SemaphoreType.DMA
    result = pl.pallas_call(
        kernel,
        out_shape=jax.ShapeDtypeStruct((2 * parent_dev, 128), jnp.float32),
        in_specs=[anywhere] * 6,
        out_specs=vmem,
        scratch_shapes=[
            pltpu.VMEM((3 * (CHIPS // 2) * THIRD, sample_cols), jnp.bfloat16),
            pltpu.VMEM((CHIPS * REST, sample_cols), jnp.bfloat16),
            pltpu.VMEM((CHIPS, local_rows, 3 * THIRD), jnp.bfloat16),
            pltpu.VMEM((CHIPS // 2, local_rows, 2 * REST), jnp.bfloat16),
            pltpu.VMEM((3 * (CHIPS // 2), local_rows, THIRD), jnp.bfloat16),
            pltpu.VMEM((local_rows, sample_cols), jnp.float32),
            pltpu.VMEM((3, local_rows, sample_cols), jnp.float32),
            pltpu.VMEM((3, local_rows, sample_cols), jnp.float32),
            pltpu.VMEM((2 * parent_dev, 128), jnp.float32),
            pltpu.VMEM((slot_rows, 256), jnp.bfloat16),
            tiles,
            tiles,
            tiles,
            tiles,
            pltpu.VMEM((slot_rows, local_rows), jnp.bfloat16),
            pltpu.VMEM((parent_dev, slot_rows), jnp.bfloat16),
            pltpu.VMEM((slot_rows, parent_dev), jnp.bfloat16),
            pltpu.VMEM((parent_dev, slot_rows), jnp.bfloat16),
            pltpu.VMEM((parent_dev, leaf_size), jnp.bfloat16),
            pltpu.VMEM((parent_dev, sample_cols), jnp.bfloat16),
            pltpu.VMEM(child_map.shape, jnp.int32),
            pltpu.VMEM((parent_dev, 128), jnp.int32),
            pltpu.VMEM((OWNERS // 2, 2 * local_rows), jnp.int32),
            pltpu.VMEM((2 * CAP, OWNERS, 128), jnp.float32),
            pltpu.VMEM((128, parent_dev), jnp.float32),
            dma((4,)),
            dma((CHIPS,)),
            dma((CHIPS // 2,)),
            dma((4,)),
            dma((6,)),
            dma((2, 3)),
            dma((len(steps),)),
            pltpu.SemaphoreType.REGULAR,
            dma((2,)),
            dma((2,)),
            dma((2,)),
            dma((2,)),
        ],
        compiler_params=pltpu.CompilerParams(
            collective_id=0, has_side_effects=True, vmem_limit_bytes=67043328
        ),
    )(front_update, child_omega, parent_block, parent_omega, child_map, leaf_order.reshape(parent_dev, 128))
    return jnp.concatenate([result[:parent_dev], result[parent_dev:]], axis=1)


def solution(mesh):
    placed = (
        P("child", "rows", None),
        P("child", "rows", None),
        P(("child", "rows"), None),
        P(("child", "rows"), None),
        P(),
        P(),
    )
    return jax.shard_map(
        body, mesh=mesh, in_specs=placed, out_specs=P(("child", "rows"), None), check_vma=False
    )
```
